512 devices in a mesh: groups: 2 (over y), parts: 32 (over z), sub: 4 (over x), pair: 2 (over core).
Axes of the slice: x: 4, y: 2, z: 32, core: 2. Of those that a mesh axis runs over, the one named last changes fastest.
The devices are a block of a 4x8x32 slice.
Arguments:
- spectra: bfloat16 [2048, 128, 128], P(('groups', 'parts', 'pair')), parts along dimension 0, may hold values from -6 to 6
- defocus: bfloat16 [2048], P(('groups', 'parts', 'pair')), parts along dimension 0, may hold values from 0.5 to 2
- classes: int32 [2048, 4], P(('groups', 'parts', 'pair')), parts along dimension 0, may hold values from 0 to 31, all different within a row
- poses: int32 [2048, 4], P(('groups', 'parts', 'pair')), parts along dimension 0, may hold values from 0 to 31
- probs: bfloat16 [2048, 4], P(('groups', 'parts', 'pair')), parts along dimension 0, may hold values from 0.049804688 to 1
- counts: int32 [128], P(('groups', 'parts', 'pair')), parts along dimension 0, may hold values from 1 to 16, as said below
- offsets: int32 [32], replicated, may hold values from 0 to 64
- row_kernel: bfloat16 [32, 256, 64], P(None, 'sub'), may hold values from -0.015625 to 0.046875
- col_kernel: bfloat16 [32, 128, 64], replicated, may hold values from -0.015625 to 0.046875
Outputs:
- averages: float32 [64, 256, 256], P('groups', ('sub', 'pair')), parts along dimension 0
The draws below stay inside these ranges and needn't reach their ends.
There are 2 independent parts, one for each index of `groups`. The reference program is written for one: setup_inputs(seed, part) draws one part's arguments, and reference() takes and returns one part's arrays. A program takes and returns all parts, laid end to end along the dimension named above; an argument that names none is the same for every part. Nothing has to cross between parts.
Inputs may be any that keep to these rules, and one draw needn't show every extreme that they name: Only the first counts slots of a shard hold used particles; some shard uses all 16 slots. The 4 classes of a particle differ.
All inputs are finite; a program needn't handle non-finite values.
Results may differ from the reference program's by a relative error of at most 0.0038.
Values may be sent and summed in bfloat16 or wider, within the bound.
No kernel may reach another device: no remote copies, remote signals or barrier semaphores. Data moves between devices by JAX's collectives and lax.ppermute only.
A program may use at most 64 MiB of HBM per device.

```python
import math
import jax
import jax.numpy as jnp
from jax import lax

GRID = 512
BOX = 256
IROWS = 128
ICOLS = 64
LROWS = 256
LCOLS = 128
BAND = 64
NPOSE = 32
K_TOP = 4
ITERS = 4
P_DEV = 16
SHARDS = 64
PARTICLES = 1024
CLASSES = 32
N_PARTS = 32
N_PAIR = 2


def draw_counts(key, part):
    first_key, second_key = jax.random.split(jax.random.fold_in(key, 11))
    drawn = jax.random.randint(first_key, (SHARDS,), 1, P_DEV + 1)
    full_shard = jax.random.randint(second_key, (), 0, SHARDS)
    return jnp.where(jnp.arange(SHARDS) == full_shard, P_DEV, drawn).astype(jnp.int32)


def touch_ends(values, rng, smallest, top_value):
    longest = values.shape.index(max(values.shape))
    spots = []
    for shift in (0, 1):
        where = [jax.random.randint(jax.random.fold_in(rng, axis), (), 0, length) for axis, length in enumerate(values.shape)]
        where[longest] = (where[longest] + shift) % values.shape[longest]
        spots.append(tuple(where))
    return values.at[spots[0]].set(smallest).at[spots[1]].set(top_value)


def shard_levels(stream_key, extent, shards, smallest, high):
    loudness = 1.0
    for dim, parts in shards:
        steps = jax.random.uniform(jax.random.fold_in(jax.random.fold_in(stream_key, 6), dim), (parts,), jnp.float32, smallest / len(shards), high / len(shards))
        loudness = loudness * jnp.repeat(jnp.exp(steps), extent[dim] // parts).reshape((-1,) + (1,) * (len(extent) - 1 - dim))
    return loudness


def picks_of(own_key, rows, count, top, lift):
    sequence = jax.random.permutation(jax.random.fold_in(own_key, 1), count)
    pull = sequence
    for power in range(3):
        pull = pull * pull // count
    pull = pull * lift // count
    lots = jax.random.randint(jax.random.fold_in(own_key, 2), (rows, count), 0, 4096) + pull
    sure = jax.random.permutation(jax.random.fold_in(own_key, 3), rows)[jnp.arange(count) % rows]
    lots = jnp.where(jnp.arange(rows)[:, None] == sure[None, :], 1 << 14, lots)
    merit = lots * count + jnp.arange(count)
    return lax.top_k(merit.astype(jnp.int32), top)[1].astype(jnp.int32)


def scatter_about(key, shape, width, most, cuts=(), held_as=jnp.bfloat16):
    result = jax.random.normal(key, shape, jnp.float32) * width
    if len(cuts) > 0:
        result = shard_levels(key, shape, cuts, -0.22, 0.18) * result
    return jnp.clip(result, min=-most, max=most).astype(held_as)


def setup_inputs(seed: int = 0, part: int = 0) -> dict:
    key_of = jax.random.split(jax.random.key(seed), 10)
    part_keys = jax.random.split(jax.random.fold_in(key_of[9], part), 10)
    spectra = scatter_about(part_keys[0], (PARTICLES, IROWS, 2 * ICOLS), 1.0, 6.0, ((0, 64),))
    defocus = jnp.clip(jnp.exp(math.log(2.0) - 1.3862944 * jax.random.uniform(part_keys[1], (PARTICLES,), jnp.float32) ** shard_levels(part_keys[1], (PARTICLES,), ((0, 64),), -0.2, 0.2)), 0.5, 2.0).astype(jnp.bfloat16)
    classes = picks_of(part_keys[2], PARTICLES, CLASSES, K_TOP, 2048)
    poses = touch_ends(jax.random.randint(part_keys[3], (PARTICLES, K_TOP), 0, NPOSE), jax.random.fold_in(part_keys[3], 1), 0, NPOSE - 1).astype(jnp.int32)
    probs = jnp.clip(jnp.exp(math.log(1.0) - 2.9996462 * jax.random.uniform(part_keys[4], (PARTICLES, K_TOP), jnp.float32) ** shard_levels(part_keys[4], (PARTICLES, K_TOP), ((0, 64),), -0.2, 0.2)), 0.049804688, 1.0).astype(jnp.bfloat16)
    counts = draw_counts(jax.random.fold_in(jax.random.fold_in(key_of[9], part), 71), part)
    offsets = touch_ends(jax.random.randint(key_of[6], (NPOSE,), 0, IROWS - BAND + 1), jax.random.fold_in(key_of[6], 1), 0, IROWS - BAND).astype(jnp.int32)
    row_kernel = jnp.clip(-0.015625 + 0.0625 * jax.random.uniform(key_of[7], (NPOSE, LROWS, BAND), jnp.float32) ** shard_levels(key_of[7], (NPOSE, LROWS, BAND), ((1, 4),), -0.2, 0.2), -0.015625, 0.046875).astype(jnp.bfloat16)
    col_kernel = jnp.clip(jax.random.uniform(key_of[8], (NPOSE, LCOLS, ICOLS), jnp.float32, -0.015625, 0.046875), -0.015625, 0.046875).astype(jnp.bfloat16)
    return dict(spectra=spectra, defocus=defocus, classes=classes, poses=poses, probs=probs, counts=counts, offsets=offsets, row_kernel=row_kernel, col_kernel=col_kernel)


blob_width = 1.5
avg_scale = 8.0
floor_value = 1.0

def ctf_planes(spec_block, defocus_block):
    row_freq = jnp.arange(IROWS, dtype=jnp.float32) - IROWS // 2
    col_freq = jnp.arange(ICOLS, dtype=jnp.float32)
    radius = (row_freq[:, None] ** 2 + col_freq[None, :] ** 2) / (ICOLS * ICOLS)
    phases = 20.0 * math.pi * defocus_block.astype(jnp.float32)[:, None, None] * radius[None] + 0.1
    ctf_value = jnp.sin(phases)
    real_plane = ctf_value * spec_block[:, :, :ICOLS].astype(jnp.float32)
    imag_plane = ctf_value * spec_block[:, :, ICOLS:].astype(jnp.float32)
    return jnp.concatenate([real_plane, imag_plane, ctf_value * ctf_value], axis=2).astype(jnp.bfloat16)

def window_rows(plane_set, start_set):
    return jax.vmap(lambda row_start: lax.dynamic_slice_in_dim(plane_set, row_start, BAND, 0))(start_set)

def block_terms(planes, weights, pose_block, offsets, row_kernel, col_kernel):
    row_starts = offsets[pose_block].astype(jnp.int32)
    windows = jax.vmap(window_rows)(planes, row_starts)
    rows_k = row_kernel[pose_block].astype(jnp.float32)
    cols_k = col_kernel[pose_block].astype(jnp.float32)
    mixed_rows = jnp.einsum('nkrb,nkbj->nkrj', rows_k, windows.astype(jnp.float32), precision=lax.Precision.HIGHEST)
    mixed_rows = (mixed_rows * weights[:, :, None, None]).astype(jnp.bfloat16)
    shape_set = mixed_rows.shape
    mixed_rows = mixed_rows.reshape(shape_set[0], shape_set[1], shape_set[2], 3, ICOLS)
    spread = jnp.einsum('nkrpi,nkci->nkrpc', mixed_rows.astype(jnp.float32), cols_k, precision=lax.Precision.HIGHEST)
    return spread.reshape(shape_set[0] * shape_set[1], shape_set[2], 3 * LCOLS)

def limit_rows():
    return ((jnp.arange(LROWS, dtype=jnp.int32) - LROWS // 2) % GRID).astype(jnp.int32)

def space_from(freq_real, freq_imag):
    row_index = limit_rows()
    col_factor = jnp.where(jnp.arange(LCOLS) == 0, 1.0, 2.0).astype(jnp.float32)
    real_full = jnp.zeros((GRID, GRID), jnp.float32).at[row_index, :LCOLS].set(freq_real * col_factor[None, :])
    imag_full = jnp.zeros((GRID, GRID), jnp.float32).at[row_index, :LCOLS].set(freq_imag * col_factor[None, :])
    return jnp.real(jnp.fft.ifft2(lax.complex(real_full, imag_full))) * GRID

def freq_from(image_field):
    full_freq = jnp.fft.fft2(image_field) / GRID
    picked = full_freq[limit_rows(), :LCOLS]
    return (jnp.real(picked), jnp.imag(picked))

def refine(class_grid):
    grid_index = jnp.arange(GRID, dtype=jnp.int32)
    distance = jnp.minimum(grid_index, GRID - grid_index).astype(jnp.float32)
    blob_axis = jnp.exp(-2.0 * math.pi * math.pi * blob_width * blob_width * distance * distance / (GRID * GRID))
    blob_grid = blob_axis[:, None] * blob_axis[None, :]
    weight_plane = class_grid[:, 2 * LCOLS:]
    rescale = jnp.ones_like(weight_plane)
    for sweep_index in range(ITERS):
        image_field = space_from(weight_plane * rescale, jnp.zeros_like(weight_plane)) * blob_grid
        conv_real, conv_imag = freq_from(image_field)
        rescale = rescale / jnp.maximum(jnp.sqrt(conv_real * conv_real + conv_imag * conv_imag), floor_value)
    image_field = space_from(class_grid[:, :LCOLS] * rescale, class_grid[:, LCOLS:2 * LCOLS] * rescale)
    crop_index = jnp.arange(BOX, dtype=jnp.int32) - BOX // 2
    crop_pos = (crop_index % GRID).astype(jnp.int32)
    correction = jnp.sinc(crop_index.astype(jnp.float32) / GRID) ** 2
    picked = image_field[crop_pos][:, crop_pos]
    return picked.T * avg_scale / (correction[:, None] * correction[None, :])

def reference(spectra, defocus, classes, poses, probs, counts, offsets, row_kernel, col_kernel):
    slot_total = spectra.shape[0]
    per_device = slot_total // (N_PARTS * N_PAIR)
    slot_index = jnp.arange(slot_total, dtype=jnp.int32)
    used_slot = slot_index % per_device < counts[slot_index // per_device]
    weights = probs.astype(jnp.float32) * used_slot.astype(jnp.float32)[:, None]

    def add_block(class_grids, block_index):
        first_slot = (block_index * 8).astype(jnp.int32)
        spec_block = lax.dynamic_slice_in_dim(spectra, first_slot, 8, 0)
        defocus_block = lax.dynamic_slice_in_dim(defocus, first_slot, 8, 0)
        weight_block = lax.dynamic_slice_in_dim(weights, first_slot, 8, 0)
        pose_block = lax.dynamic_slice_in_dim(poses, first_slot, 8, 0)
        class_block = lax.dynamic_slice_in_dim(classes, first_slot, 8, 0)
        planes = ctf_planes(spec_block, defocus_block)
        insert_terms = block_terms(planes, weight_block, pose_block, offsets, row_kernel, col_kernel)
        return (class_grids.at[class_block.reshape(-1)].add(insert_terms), None)
    empty_grid = jnp.zeros((CLASSES, LROWS, 3 * LCOLS), jnp.float32)
    class_grids, unused = lax.scan(add_block, empty_grid, jnp.arange(slot_total // 8, dtype=jnp.int32))
    return lax.map(refine, class_grids)
```

```python
import functools
import math

import jax
import jax.numpy as jnp
import numpy as np
from jax import lax
from jax.experimental import pallas as pl
from jax.experimental.pallas import tpu as pltpu
from jax.sharding import PartitionSpec as P

GRID = 512
BOX = 256
IROWS = 128
ICOLS = 64
LROWS = 256
LCOLS = 128
BAND = 64
K_TOP = 4
ITERS = 4
LANES = 128
UNROLL = 4
WEIGHTS, DEFOCUS, CLASSES, POSES, COUNT, CORE = 0, K_TOP, K_TOP + 1, 2 * K_TOP + 1, 3 * K_TOP + 1, 3 * K_TOP + 2

blob_width = 1.5
avg_scale = 8.0
floor_value = 1.0

F32 = jnp.float32
BF16 = jnp.bfloat16
NT = (((1,), (1,)), ((), ()))
NN = (((1,), (0,)), ((), ()))


def sine_terms():
    r = np.cos(np.linspace(0.0, np.pi, 4001)) * 0.5
    r = r[np.abs(r) > 1e-3]
    z = r * r
    powers = np.stack([z**k for k in range(6)], axis=1)
    terms, *_ = np.linalg.lstsq(powers, np.sin(np.pi * r) / r, rcond=None)
    return [float(t) for t in terms]


SINE = sine_terms()


def particle_kernel(own, pack_ref, offsets_ref, spec_ref, rk_ref, ck_ref, *rest):
    grid_in, grid_ref, placed_ref, radius_ref = rest if len(rest) == 4 else (None, *rest)
    n_pose, half = rk_ref.shape[0], rk_ref.shape[1] // 2
    count = pack_ref[COUNT, 0].astype(jnp.int32)
    core = pack_ref[CORE, 0].astype(jnp.int32)
    first_row = pl.multiple_of((core if own else 1 - core) * half, half)

    lane = lax.broadcasted_iota(jnp.int32, (1, LANES), 1)
    low = lane < ICOLS
    row_freq = (lax.broadcasted_iota(jnp.int32, (IROWS, LANES), 0) - IROWS // 2).astype(F32)
    col_freq = (lax.broadcasted_iota(jnp.int32, (IROWS, LANES), 1) & (ICOLS - 1)).astype(F32)
    radius_ref[...] = (row_freq * row_freq + col_freq * col_freq) * (10.0 / (ICOLS * ICOLS))

    def place(b, carry):
        rows = rk_ref[b, pl.ds(first_row, half), :].astype(F32)
        rows = jnp.concatenate([rows, jnp.zeros((half, LANES - BAND), F32)], axis=1)
        placed_ref[b] = pltpu.roll(rows, offsets_ref[b], 1).astype(BF16)
        return carry

    lax.fori_loop(0, n_pose, place, 0)
    if grid_in is None:
        grid_ref[...] = jnp.zeros_like(grid_ref)
    else:
        grid_ref[...] = grid_in[...]

    def step(block, carry):
        sums = []
        for u in range(UNROLL):
            n = block * UNROLL + u
            turns = radius_ref[...] * pack_ref[DEFOCUS, n]
            turns = turns - jnp.floor(turns + 0.5)
            t = 2.0 * turns + 0.1 / math.pi
            k = jnp.floor(t + 0.5)
            r = t - k
            z = r * r
            s = SINE[-1]
            for term in SINE[-2::-1]:
                s = s * z + term
            ctf = s * r * (1.0 - 2.0 * k * k)
            data = (ctf * spec_ref[n].astype(F32)).astype(BF16)
            power = jnp.where(low, ctf * ctf, 0.0).astype(BF16)
            planes = jnp.concatenate([data, power], axis=1)
            poses = [pack_ref[POSES + j, n].astype(jnp.int32) for j in range(K_TOP)]
            rows = jnp.concatenate([placed_ref[b] for b in poses], axis=0)
            mixed = lax.dot_general(rows, planes, NN, preferred_element_type=F32)
            for j in range(K_TOP):
                m = mixed[j * half : (j + 1) * half] * pack_ref[WEIGHTS + j, n]
                pair = m[:, :LANES]
                stacked = jnp.concatenate(
                    [jnp.where(low, pair, 0.0), jnp.where(low, 0.0, pair), m[:, LANES:]], axis=0
                ).astype(BF16)
                cols = ck_ref[poses[j]]
                cols = jnp.concatenate([cols, cols], axis=0)
                spread = lax.dot_general(stacked, cols, NN, preferred_element_type=F32)
                sums.append((pack_ref[CLASSES + j, n].astype(jnp.int32), spread))
        for c, spread in sums:
            grid_ref[c] += spread
        return carry

    lax.fori_loop(0, (count + UNROLL - 1) // UNROLL, step, 0)


def insert_particles(pack, offsets, spectra, row_kernel, col_kernel, n_class, grids=None):
    n_pose, rows, _ = row_kernel.shape
    out = (n_class, 3 * (rows // 2), LCOLS)
    smem = pl.BlockSpec(memory_space=pltpu.SMEM)
    vmem = pl.BlockSpec(memory_space=pltpu.VMEM)
    operands = [pack, offsets, spectra, row_kernel, col_kernel]
    if grids is not None:
        operands.append(grids)
    work = spectra.shape[0] * K_TOP * (rows // 2) * 2
    return pl.pallas_call(
        functools.partial(particle_kernel, grids is None),
        out_shape=jax.ShapeDtypeStruct(out, F32),
        in_specs=[smem, smem] + [vmem] * (len(operands) - 2),
        out_specs=vmem,
        scratch_shapes=[
            pltpu.VMEM((n_pose, rows // 2, LANES), BF16),
            pltpu.VMEM((IROWS, LANES), F32),
        ],
        cost_estimate=pl.CostEstimate(
            flops=work * (IROWS * 2 * LANES + 3 * LANES * LCOLS) * 8,
            bytes_accessed=2 * 4 * math.prod(out),
            transcendentals=0,
        ),
        compiler_params=pltpu.CompilerParams(vmem_limit_bytes=32 * 2**20),
        name="insert_particles",
    )(*operands)


def split_bf16(x):
    hi = x.astype(BF16)
    return hi, (x - hi.astype(F32)).astype(BF16)


def dot3(a, b, dims):
    (ah, al), (bh, bl) = a, b
    dot = functools.partial(lax.dot_general, dimension_numbers=dims, preferred_element_type=F32)
    return dot(ah, bh) + (dot(ah, bl) + dot(al, bh))


@functools.cache
def tables(groups):
    grid = np.arange(GRID)
    distance = np.minimum(grid, GRID - grid).astype(np.float64)
    blob = np.exp(-2.0 * np.pi**2 * blob_width**2 * distance**2 / GRID**2)
    angle = 2.0 * np.pi / GRID
    kernel = np.cos(angle * (grid[:, None] * grid[None, :] % GRID)) @ blob / GRID
    rows = np.arange(LROWS) - LROWS // 2
    cols = np.arange(LCOLS)
    factor = np.where(cols == 0, 1.0, 2.0)
    mix_rows = np.concatenate(
        [kernel[(rows[:, None] - rows[None, :]) % GRID], kernel[(rows[:, None] + rows[None, :]) % GRID]], axis=1
    )
    half = 0.5 * factor[:, None]
    mix_cols = np.concatenate(
        [half * kernel[(cols[:, None] - cols[None, :]) % GRID], half * kernel[(cols[:, None] + cols[None, :]) % GRID]],
        axis=1,
    )
    crop = np.arange(BOX) - BOX // 2
    correction = np.sinc(crop / GRID) ** 2
    row_angle = angle * (rows[:, None] * crop[None, :] % GRID)
    last_rows = np.concatenate([np.cos(row_angle), -np.sin(row_angle)], axis=0)
    last_rows = last_rows * (avg_scale / GRID) / correction[None, :]
    col_angle = angle * (crop[:, None] * cols[None, :] % GRID)
    last_cols = np.stack([np.cos(col_angle), np.sin(col_angle)], axis=0)
    last_cols = last_cols * factor[None, None, :] / correction[None, :, None]
    last_cols = last_cols.reshape(2, groups, BOX // groups, LCOLS).transpose(1, 0, 2, 3)
    last_cols = last_cols.reshape(groups, 2 * (BOX // groups), LCOLS)

    def two(x):
        x = x.astype(np.float32)
        hi = x.astype(jnp.bfloat16)
        lo = (x - hi.astype(np.float32)).astype(jnp.bfloat16)
        return np.stack([hi, lo])

    return two(mix_rows), two(mix_cols), two(last_rows), two(last_cols)


def refine_kernel(planes_ref, mix_rows_ref, mix_cols_ref, last_rows_ref, last_cols_ref, out_ref):
    blocks, third = planes_ref.shape[0], planes_ref.shape[1] // 3

    def plane(p):
        return jnp.concatenate([planes_ref[g, p * third : (p + 1) * third] for g in range(blocks)], axis=0).astype(F32)

    weight = plane(2)
    mix_rows = (mix_rows_ref[0], mix_rows_ref[1])
    mix_cols = (mix_cols_ref[0], mix_cols_ref[1])
    scale = jnp.ones_like(weight)
    for _ in range(ITERS):
        half = dot3(split_bf16(weight * scale), mix_cols, NN)
        half = jnp.concatenate([half[:, :LCOLS], half[:, LCOLS:]], axis=0)
        conv = dot3(mix_rows, split_bf16(half), NN)
        scale = scale / jnp.maximum(jnp.abs(conv), floor_value)
    last_cols = (last_cols_ref[0], last_cols_ref[1])
    real = dot3(last_cols, split_bf16(plane(0) * scale), NT)
    imag = dot3(last_cols, split_bf16(plane(1) * scale), NT)
    n = real.shape[0] // 2
    both = jnp.concatenate([real[:n] - imag[n:], real[n:] + imag[:n]], axis=1)
    out = dot3(split_bf16(both), (last_rows_ref[0], last_rows_ref[1]), NN)
    out_ref[...] = out.astype(out_ref.dtype)


def refine_class(planes, mix_rows, mix_cols, last_rows, last_cols):
    vmem = pl.BlockSpec(memory_space=pltpu.VMEM)
    return pl.pallas_call(
        refine_kernel,
        out_shape=jax.ShapeDtypeStruct((last_cols.shape[1] // 2, BOX), BF16),
        in_specs=[vmem] * 5,
        out_specs=vmem,
        cost_estimate=pl.CostEstimate(flops=2 * 10**9, bytes_accessed=3 * 10**6, transcendentals=0),
        compiler_params=pltpu.CompilerParams(vmem_limit_bytes=32 * 2**20),
        name="refine_class",
    )(planes, mix_rows, mix_cols, last_rows, last_cols)


def shift(value, axis, by):
    n = lax.axis_size(axis)
    return lax.ppermute(value, axis, [(i, (i + by) % n) for i in range(n)])


def sum_at_owner(parts, axis):
    here = lax.all_to_all(parts.astype(BF16), axis, split_axis=0, concat_axis=0, tiled=True)
    return jnp.sum(here.astype(F32), axis=0)


def per_device(spectra, defocus, classes, poses, probs, counts, offsets, row_kernel, col_kernel):
    n_slots = spectra.shape[0]
    n_class = lax.axis_size("parts")
    group = lax.axis_size("sub") * lax.axis_size("pair")
    used = (jnp.arange(n_slots, dtype=jnp.int32) < counts[0]).astype(F32)
    pack = jnp.concatenate(
        [
            probs.T.astype(F32) * used[None],
            defocus.astype(F32)[None],
            classes.T.astype(F32),
            poses.T.astype(F32),
            jnp.broadcast_to(counts.astype(F32)[:, None], (1, n_slots)),
            jnp.broadcast_to(lax.axis_index("pair").astype(F32), (1, n_slots)),
        ],
        axis=0,
    )
    other_pack = shift(pack, "pair", 1)
    other_spectra = shift(spectra, "pair", 1)
    kernels = (row_kernel, jnp.swapaxes(col_kernel, 1, 2))
    grids = insert_particles(pack, offsets, spectra, *kernels, n_class)
    grids = insert_particles(other_pack, offsets, other_spectra, *kernels, n_class, grids)
    own = sum_at_owner(grids, "parts")
    planes = lax.all_gather(own, ("sub", "pair"), axis=0, tiled=False)
    mix_rows, mix_cols, last_rows, last_cols = tables(group)
    mine = lax.dynamic_index_in_dim(jnp.asarray(last_cols), lax.axis_index(("sub", "pair")), 1, keepdims=False)
    average = refine_class(planes, jnp.asarray(mix_rows), jnp.asarray(mix_cols), jnp.asarray(last_rows), mine)
    return lax.all_gather(average, "parts", axis=0, tiled=False).astype(F32)


def solution(mesh):
    shards = ("groups", "parts", "pair")
    placed = (
        P(shards, None, None),
        P(shards),
        P(shards, None),
        P(shards, None),
        P(shards, None),
        P(shards),
        P(),
        P(None, "sub", None),
        P(),
    )
    return jax.shard_map(
        per_device,
        mesh=mesh,
        in_specs=placed,
        out_specs=P("groups", ("sub", "pair"), None),
        check_vma=False,
    )
```

```python
import functools
import math

import jax
import jax.numpy as jnp
import numpy as np
from jax import lax
from jax.experimental import pallas as pl
from jax.experimental.pallas import tpu as pltpu
from jax.sharding import PartitionSpec as P

GRID = 512
BOX = 256
IROWS = 128
ICOLS = 64
LROWS = 256
LCOLS = 128
BAND = 64
K_TOP = 4
ITERS = 4
LANES = 128
UNROLL = 4
ALL_VMEM = 67043328
WEIGHTS, DEFOCUS, CLASSES, POSES, COUNT, SMALL = 0, K_TOP, K_TOP + 1, 2 * K_TOP + 1, 3 * K_TOP + 1, 16
NEAR = 4
FAR = 8

blob_width = 1.5
avg_scale = 8.0
floor_value = 1.0

F32 = jnp.float32
BF16 = jnp.bfloat16
NT = (((1,), (1,)), ((), ()))
NN = (((1,), (0,)), ((), ()))


def sine_terms():
    r = np.cos(np.linspace(0.0, np.pi, 4001)) * 0.5
    r = r[np.abs(r) > 1e-3]
    z = r * r
    powers = np.stack([z**k for k in range(6)], axis=1)
    terms, *_ = np.linalg.lstsq(powers, np.sin(np.pi * r) / r, rcond=None)
    return [float(t) for t in terms]


SINE = sine_terms()


def start_all(pairs, sems):
    copies = [pltpu.make_async_copy(source, target, sems.at[i]) for i, (source, target) in enumerate(pairs)]
    for copy in copies:
        copy.start()
    return copies


def prepare_kernel(
    counts_in, probs_in, defocus_in, classes_in, poses_in, spec_in,
    pages_ref, counts_ref, probs_ref, defocus_ref, classes_ref, poses_ref, small_ref, sems,
):
    n_slots = spec_in.shape[0]
    copies = start_all(
        [
            (spec_in, pages_ref.at[pl.ds(0, n_slots)]),
            (counts_in, counts_ref),
            (probs_in, probs_ref),
            (defocus_in, defocus_ref),
            (classes_in, classes_ref),
            (poses_in, poses_ref),
        ],
        sems,
    )
    small_ref[...] = jnp.zeros_like(small_ref)
    pages_ref[n_slots] = jnp.zeros(pages_ref.shape[1:], BF16)
    for copy in copies[1:]:
        copy.wait()
    used = lax.broadcasted_iota(jnp.int32, (K_TOP, n_slots), 1) < counts_ref[0]
    small_ref[WEIGHTS : WEIGHTS + K_TOP, :n_slots] = jnp.where(used, probs_ref[...].astype(F32), 0.0)
    small_ref[DEFOCUS : DEFOCUS + 1, :n_slots] = defocus_ref[...].astype(F32)
    small_ref[CLASSES : CLASSES + K_TOP, :n_slots] = classes_ref[...].astype(F32)
    small_ref[POSES : POSES + K_TOP, :n_slots] = poses_ref[...].astype(F32)
    small_ref[COUNT : COUNT + 1, :] = jnp.full((1, LANES), counts_ref[0], jnp.int32).astype(F32)
    pages_ref[n_slots, :SMALL] = small_ref[...].astype(BF16)
    copies[0].wait()


def prepare(counts, probs, defocus, classes, poses, spectra):
    n_slots = spectra.shape[0]
    return pl.pallas_call(
        prepare_kernel,
        out_shape=jax.ShapeDtypeStruct((n_slots + 1, IROWS, LANES), BF16),
        in_specs=[pl.BlockSpec(memory_space=pl.ANY)] * 6,
        out_specs=pl.BlockSpec(memory_space=pltpu.VMEM),
        scratch_shapes=[
            pltpu.SMEM(counts.shape, jnp.int32),
            pltpu.VMEM(probs.shape, BF16),
            pltpu.VMEM(defocus.shape, BF16),
            pltpu.VMEM(classes.shape, jnp.int32),
            pltpu.VMEM(poses.shape, jnp.int32),
            pltpu.VMEM((SMALL, LANES), F32),
            pltpu.SemaphoreType.DMA((6,)),
        ],
        cost_estimate=pl.CostEstimate(flops=10**6, bytes_accessed=2 * 10**6, transcendentals=0),
        compiler_params=pltpu.CompilerParams(vmem_limit_bytes=ALL_VMEM),
        name="prepare",
    )(counts, probs, defocus, classes, poses, spectra)


def particle_kernel(
    spread_over, core_ref, offsets_in, rk_in, ck_in, own_in, other_in,
    out_ref, offsets_ref, rows_ref, cols_ref, pages_ref, placed_ref, total_ref, radius_ref, small_ref, scalars_ref, sems,
):
    n_slots = pages_ref.shape[1] - 1
    n_pose, half = placed_ref.shape[0], placed_ref.shape[1]
    first_row = pl.multiple_of(core_ref[0] * half, half)
    copies = start_all(
        [
            (offsets_in, offsets_ref),
            (rk_in.at[:, pl.ds(first_row, half), :], rows_ref),
            (own_in, pages_ref.at[0]),
            (other_in, pages_ref.at[1]),
            (ck_in, cols_ref),
        ],
        sems,
    )
    lane = lax.broadcasted_iota(jnp.int32, (1, LANES), 1)
    low = lane < ICOLS
    row_freq = (lax.broadcasted_iota(jnp.int32, (IROWS, LANES), 0) - IROWS // 2).astype(F32)
    col_freq = (lax.broadcasted_iota(jnp.int32, (IROWS, LANES), 1) & (ICOLS - 1)).astype(F32)
    radius_ref[...] = (row_freq * row_freq + col_freq * col_freq) * (10.0 / (ICOLS * ICOLS))
    total_ref[...] = jnp.zeros_like(total_ref)
    copies[0].wait()
    copies[1].wait()
    for b in range(n_pose):
        band = rows_ref[b].astype(F32)
        band = jnp.concatenate([band, jnp.zeros((half, LANES - BAND), F32)], axis=1)
        placed_ref[b] = pltpu.roll(band, offsets_ref[b], 1).astype(BF16)
    copies[2].wait()
    copies[3].wait()
    small_ref[...] = pages_ref[:, n_slots, :SMALL].astype(F32)
    scalars = pltpu.make_async_copy(small_ref, scalars_ref, sems.at[5])
    scalars.start()
    copies[4].wait()
    scalars.wait()

    def pick(shard, row, n):
        return scalars_ref[shard, row, n].astype(jnp.int32)

    blocks = [(pick(shard, COUNT, 0) + UNROLL - 1) // UNROLL for shard in range(2)]

    def step(block, carry):
        shard = (block >= blocks[0]).astype(jnp.int32)
        first = (block - shard * blocks[0]) * UNROLL
        sums = []
        for u in range(UNROLL):
            n = first + u
            turns = radius_ref[...] * scalars_ref[shard, DEFOCUS, n]
            turns = turns - jnp.floor(turns + 0.5)
            t = 2.0 * turns + 0.1 / math.pi
            k = jnp.floor(t + 0.5)
            r = t - k
            z = r * r
            s = SINE[-1]
            for term in SINE[-2::-1]:
                s = s * z + term
            ctf = s * r * (1.0 - 2.0 * k * k)
            data = (ctf * pages_ref[shard, n].astype(F32)).astype(BF16)
            power = jnp.where(low, ctf * ctf, 0.0).astype(BF16)
            planes = jnp.concatenate([data, power], axis=1)
            poses = [pick(shard, POSES + j, n) for j in range(K_TOP)]
            rows = jnp.concatenate([placed_ref[b] for b in poses], axis=0)
            mixed = lax.dot_general(rows, planes, NN, preferred_element_type=F32)
            for j in range(K_TOP):
                m = mixed[j * half : (j + 1) * half] * scalars_ref[shard, WEIGHTS + j, n]
                pair = m[:, :LANES]
                stacked = jnp.concatenate(
                    [jnp.where(low, pair, 0.0), jnp.where(low, 0.0, pair), m[:, LANES:]], axis=0
                ).astype(BF16)
                cols = cols_ref[poses[j]]
                cols = jnp.concatenate([cols, cols], axis=0)
                spread = lax.dot_general(stacked, cols, NN, preferred_element_type=F32)
                c = pick(shard, CLASSES + j, n)
                sums.append(((c % spread_over) * (total_ref.shape[0] // spread_over) + c // spread_over, spread))
        for c, spread in sums:
            total_ref[c] += spread
        return carry

    lax.fori_loop(0, blocks[0] + blocks[1], step, 0)
    out_ref[...] = total_ref[...].astype(out_ref.dtype)


def insert_particles(core, offsets, row_kernel, col_kernel, pages, other_pages, n_class, spread_over):
    n_pose, rows, _ = row_kernel.shape
    half = rows // 2
    out = (n_class, 3 * half, LCOLS)
    work = 2 * (pages.shape[0] - 1) * K_TOP * half * 2
    return pl.pallas_call(
        functools.partial(particle_kernel, spread_over),
        out_shape=jax.ShapeDtypeStruct(out, BF16),
        in_specs=[pl.BlockSpec(memory_space=pltpu.SMEM)] + [pl.BlockSpec(memory_space=pl.ANY)] * 5,
        out_specs=pl.BlockSpec(memory_space=pltpu.VMEM),
        scratch_shapes=[
            pltpu.SMEM(offsets.shape, jnp.int32),
            pltpu.VMEM((n_pose, half, BAND), BF16),
            pltpu.VMEM(col_kernel.shape, BF16),
            pltpu.VMEM((2, *pages.shape), BF16),
            pltpu.VMEM((n_pose, half, LANES), BF16),
            pltpu.VMEM(out, F32),
            pltpu.VMEM((IROWS, LANES), F32),
            pltpu.VMEM((2, SMALL, LANES), F32),
            pltpu.SMEM((2, SMALL, LANES), F32),
            pltpu.SemaphoreType.DMA((6,)),
        ],
        cost_estimate=pl.CostEstimate(
            flops=work * (IROWS * 2 * LANES + 3 * LANES * LCOLS) * 8,
            bytes_accessed=2 * 2 * math.prod(out),
            transcendentals=0,
        ),
        compiler_params=pltpu.CompilerParams(vmem_limit_bytes=ALL_VMEM),
        name="insert_particles",
    )(core, offsets, row_kernel, col_kernel, pages, other_pages)


def split_bf16(x):
    hi = x.astype(BF16)
    return hi, (x - hi.astype(F32)).astype(BF16)


def dot3(a, b, dims):
    (ah, al), (bh, bl) = a, b
    dot = functools.partial(lax.dot_general, dimension_numbers=dims, preferred_element_type=F32)
    return dot(ah, bh) + (dot(ah, bl) + dot(al, bh))


@functools.cache
def tables(groups):
    grid = np.arange(GRID)
    distance = np.minimum(grid, GRID - grid).astype(np.float64)
    blob = np.exp(-2.0 * np.pi**2 * blob_width**2 * distance**2 / GRID**2)
    angle = 2.0 * np.pi / GRID
    kernel = np.cos(angle * (grid[:, None] * grid[None, :] % GRID)) @ blob / GRID
    rows = np.arange(LROWS) - LROWS // 2
    cols = np.arange(LCOLS)
    factor = np.where(cols == 0, 1.0, 2.0)
    mix_rows = np.concatenate(
        [kernel[(rows[:, None] - rows[None, :]) % GRID], kernel[(rows[:, None] + rows[None, :]) % GRID]], axis=1
    )
    half = 0.5 * factor[:, None]
    mix_cols = np.concatenate(
        [half * kernel[(cols[:, None] - cols[None, :]) % GRID], half * kernel[(cols[:, None] + cols[None, :]) % GRID]],
        axis=1,
    )
    crop = np.arange(BOX) - BOX // 2
    correction = np.sinc(crop / GRID) ** 2
    row_angle = angle * (rows[:, None] * crop[None, :] % GRID)
    last_rows = np.concatenate([np.cos(row_angle), -np.sin(row_angle)], axis=0)
    last_rows = last_rows * (avg_scale / GRID) / correction[None, :]
    col_angle = angle * (crop[:, None] * cols[None, :] % GRID)
    last_cols = np.stack([np.cos(col_angle), np.sin(col_angle)], axis=0)
    last_cols = last_cols * factor[None, None, :] / correction[None, :, None]
    last_cols = last_cols.reshape(2, groups, BOX // groups, LCOLS).transpose(1, 0, 2, 3)
    last_cols = last_cols.reshape(groups, 2 * (BOX // groups), LCOLS)

    def two(x):
        x = x.astype(np.float32)
        hi = x.astype(jnp.bfloat16)
        lo = (x - hi.astype(np.float32)).astype(jnp.bfloat16)
        return np.stack([hi, lo])

    return two(mix_rows), two(mix_cols), two(last_rows), two(last_cols)


def refine_kernel(planes_ref, mix_rows_ref, mix_cols_ref, last_rows_ref, last_cols_ref, out_ref):
    blocks, third = planes_ref.shape[0], planes_ref.shape[1] // 3

    def plane(p):
        return jnp.concatenate([planes_ref[g, p * third : (p + 1) * third] for g in range(blocks)], axis=0).astype(F32)

    weight = plane(2)
    mix_rows = (mix_rows_ref[0], mix_rows_ref[1])
    mix_cols = (mix_cols_ref[0], mix_cols_ref[1])
    scale = jnp.ones_like(weight)
    for _ in range(ITERS):
        half = dot3(split_bf16(weight * scale), mix_cols, NN)
        half = jnp.concatenate([half[:, :LCOLS], half[:, LCOLS:]], axis=0)
        conv = dot3(mix_rows, split_bf16(half), NN)
        scale = scale / jnp.maximum(jnp.abs(conv), floor_value)
    last_cols = (last_cols_ref[0], last_cols_ref[1])
    real = dot3(last_cols, split_bf16(plane(0) * scale), NT)
    imag = dot3(last_cols, split_bf16(plane(1) * scale), NT)
    n = real.shape[0] // 2
    both = jnp.concatenate([real[:n] - imag[n:], real[n:] + imag[:n]], axis=1)
    out = dot3(split_bf16(both), (last_rows_ref[0], last_rows_ref[1]), NN)
    out_ref[...] = out.astype(out_ref.dtype)


def refine_class(planes, mix_rows, mix_cols, last_rows, last_cols):
    vmem = pl.BlockSpec(memory_space=pltpu.VMEM)
    return pl.pallas_call(
        refine_kernel,
        out_shape=jax.ShapeDtypeStruct((last_cols.shape[1] // 2, BOX), BF16),
        in_specs=[vmem] * 5,
        out_specs=vmem,
        cost_estimate=pl.CostEstimate(flops=2 * 10**9, bytes_accessed=3 * 10**6, transcendentals=0),
        compiler_params=pltpu.CompilerParams(vmem_limit_bytes=32 * 2**20),
        name="refine_class",
    )(planes, mix_rows, mix_cols, last_rows, last_cols)


def shift(value, axis, by):
    n = lax.axis_size(axis)
    return lax.ppermute(value, axis, [(i, (i + by) % n) for i in range(n)])


def neighbours(n, size):
    return [[first + i for i in range(size)] for first in range(0, n, size)]


def strided(n, stride):
    return [list(range(first, n, stride)) for first in range(stride)]


def added(parts):
    total = parts[0].astype(F32)
    for i in range(1, parts.shape[0]):
        total = total + parts[i].astype(F32)
    return total


def sum_at_owner(parts, axis):
    n = lax.axis_size(axis)
    parts = parts.reshape(NEAR, n // NEAR, *parts.shape[1:])
    parts = lax.all_to_all(parts, axis, 0, 0, axis_index_groups=neighbours(n, NEAR))
    parts = added(parts).astype(BF16)
    parts = lax.all_to_all(parts, axis, 0, 0, axis_index_groups=strided(n, NEAR))
    return added(parts)


def from_all(value, axis):
    n = lax.axis_size(axis)
    far = lax.all_gather(value, axis, axis=0, axis_index_groups=strided(n, FAR))
    every = lax.all_gather(far, axis, axis=0, axis_index_groups=neighbours(n, FAR))
    return jnp.swapaxes(every, 0, 1).reshape(n, *value.shape)


def per_device(spectra, defocus, classes, poses, probs, counts, offsets, row_kernel, col_kernel):
    n_class = lax.axis_size("parts")
    group = lax.axis_size("sub") * lax.axis_size("pair")
    pages = prepare(counts, probs.T, defocus[None], classes.T, poses.T, spectra)
    other_pages = shift(pages, "pair", 1)
    core = lax.axis_index("pair").reshape(1)
    col_rows = jnp.swapaxes(col_kernel, 1, 2)
    grids = insert_particles(core, offsets, row_kernel, col_rows, pages, other_pages, n_class, NEAR)
    own = sum_at_owner(grids, "parts")
    planes = lax.all_gather(own, ("sub", "pair"), axis=0, tiled=False)
    mix_rows, mix_cols, last_rows, last_cols = tables(group)
    mine = lax.dynamic_index_in_dim(jnp.asarray(last_cols), lax.axis_index(("sub", "pair")), 1, keepdims=False)
    average = refine_class(planes, jnp.asarray(mix_rows), jnp.asarray(mix_cols), jnp.asarray(last_rows), mine)
    return from_all(average, "parts").astype(F32)


def solution(mesh):
    shards = ("groups", "parts", "pair")
    placed = (
        P(shards, None, None),
        P(shards),
        P(shards, None),
        P(shards, None),
        P(shards, None),
        P(shards),
        P(),
        P(None, "sub", None),
        P(),
    )
    return jax.shard_map(
        per_device,
        mesh=mesh,
        in_specs=placed,
        out_specs=P("groups", ("sub", "pair"), None),
        check_vma=False,
    )
```

```python
import functools
import math

import jax
import jax.numpy as jnp
import numpy as np
from jax import lax
from jax.experimental import pallas as pl
from jax.experimental.pallas import tpu as pltpu
from jax.sharding import PartitionSpec as P

GRID = 512
BOX = 256
IROWS = 128
ICOLS = 64
LROWS = 256
LCOLS = 128
BAND = 64
K_TOP = 4
ITERS = 4
LANES = 128
UNROLL = 4
ALL_VMEM = 67043328
WEIGHTS, DEFOCUS, CLASSES, POSES, COUNT, SMALL = 0, K_TOP, K_TOP + 1, 2 * K_TOP + 1, 3 * K_TOP + 1, 16
NEAR = 4

blob_width = 1.5
avg_scale = 8.0
floor_value = 1.0

F32 = jnp.float32
BF16 = jnp.bfloat16
NT = (((1,), (1,)), ((), ()))
NN = (((1,), (0,)), ((), ()))


def sine_terms():
    r = np.cos(np.linspace(0.0, np.pi, 4001)) * 0.5
    r = r[np.abs(r) > 1e-3]
    z = r * r
    powers = np.stack([z**k for k in range(6)], axis=1)
    terms, *_ = np.linalg.lstsq(powers, np.sin(np.pi * r) / r, rcond=None)
    return [float(t) for t in terms]


SINE = sine_terms()


def start_all(pairs, sems):
    copies = [pltpu.make_async_copy(source, target, sems.at[i]) for i, (source, target) in enumerate(pairs)]
    for copy in copies:
        copy.start()
    return copies


def prepare_kernel(
    counts_in, probs_in, defocus_in, classes_in, poses_in, spec_in,
    pages_ref, counts_ref, probs_ref, defocus_ref, classes_ref, poses_ref, small_ref, sems,
):
    n_slots = spec_in.shape[0]
    copies = start_all(
        [
            (spec_in, pages_ref.at[pl.ds(0, n_slots)]),
            (counts_in, counts_ref),
            (probs_in, probs_ref),
            (defocus_in, defocus_ref),
            (classes_in, classes_ref),
            (poses_in, poses_ref),
        ],
        sems,
    )
    small_ref[...] = jnp.zeros_like(small_ref)
    pages_ref[n_slots] = jnp.zeros(pages_ref.shape[1:], BF16)
    for copy in copies[1:]:
        copy.wait()
    used = lax.broadcasted_iota(jnp.int32, (K_TOP, n_slots), 1) < counts_ref[0]
    small_ref[WEIGHTS : WEIGHTS + K_TOP, :n_slots] = jnp.where(used, probs_ref[...].astype(F32), 0.0)
    small_ref[DEFOCUS : DEFOCUS + 1, :n_slots] = defocus_ref[...].astype(F32)
    small_ref[CLASSES : CLASSES + K_TOP, :n_slots] = classes_ref[...].astype(F32)
    small_ref[POSES : POSES + K_TOP, :n_slots] = poses_ref[...].astype(F32)
    small_ref[COUNT : COUNT + 1, :] = jnp.full((1, LANES), counts_ref[0], jnp.int32).astype(F32)
    pages_ref[n_slots, :SMALL] = small_ref[...].astype(BF16)
    copies[0].wait()


def prepare(counts, probs, defocus, classes, poses, spectra):
    n_slots = spectra.shape[0]
    return pl.pallas_call(
        prepare_kernel,
        out_shape=jax.ShapeDtypeStruct((n_slots + 1, IROWS, LANES), BF16),
        in_specs=[pl.BlockSpec(memory_space=pl.ANY)] * 6,
        out_specs=pl.BlockSpec(memory_space=pltpu.VMEM),
        scratch_shapes=[
            pltpu.SMEM(counts.shape, jnp.int32),
            pltpu.VMEM(probs.shape, BF16),
            pltpu.VMEM(defocus.shape, BF16),
            pltpu.VMEM(classes.shape, jnp.int32),
            pltpu.VMEM(poses.shape, jnp.int32),
            pltpu.VMEM((SMALL, LANES), F32),
            pltpu.SemaphoreType.DMA((6,)),
        ],
        cost_estimate=pl.CostEstimate(flops=10**6, bytes_accessed=2 * 10**6, transcendentals=0),
        compiler_params=pltpu.CompilerParams(vmem_limit_bytes=ALL_VMEM),
        name="prepare",
    )(counts, probs, defocus, classes, poses, spectra)


def particle_kernel(
    place_ref, offsets_in, rk_in, ck_in, own_in, other_in,
    out0_ref, out1_ref, out2_ref, out3_ref,
    offsets_ref, rows_ref, cols_ref, pages_ref, placed_ref, total_ref, radius_ref, page_ref, small_ref, scalars_ref, sems,
):
    n_slots = pages_ref.shape[1]
    n_class = total_ref.shape[0]
    n_pose, half = placed_ref.shape[0], placed_ref.shape[1]
    first_row = pl.multiple_of(place_ref[0] * half, half)
    up = NEAR - place_ref[1]
    copies = start_all(
        [
            (own_in.at[n_slots, pl.ds(0, SMALL)], page_ref.at[0]),
            (other_in.at[n_slots, pl.ds(0, SMALL)], page_ref.at[1]),
            (offsets_in, offsets_ref),
            (rk_in.at[:, pl.ds(first_row, half), :], rows_ref),
            (own_in.at[pl.ds(0, n_slots)], pages_ref.at[0]),
            (ck_in, cols_ref),
            (other_in.at[pl.ds(0, n_slots)], pages_ref.at[1]),
        ],
        sems,
    )
    lane = lax.broadcasted_iota(jnp.int32, (1, LANES), 1)
    low = lane < ICOLS
    row_freq = (lax.broadcasted_iota(jnp.int32, (IROWS, LANES), 0) - IROWS // 2).astype(F32)
    col_freq = (lax.broadcasted_iota(jnp.int32, (IROWS, LANES), 1) & (ICOLS - 1)).astype(F32)
    radius_ref[...] = (row_freq * row_freq + col_freq * col_freq) * (10.0 / (ICOLS * ICOLS))
    total_ref[...] = jnp.zeros_like(total_ref)
    copies[0].wait()
    copies[1].wait()
    small_ref[...] = page_ref[...].astype(F32)
    scalars = pltpu.make_async_copy(small_ref, scalars_ref, sems.at[7])
    scalars.start()
    copies[2].wait()
    copies[3].wait()
    for b in range(n_pose):
        band = rows_ref[b].astype(F32)
        band = jnp.concatenate([band, jnp.zeros((half, LANES - BAND), F32)], axis=1)
        placed_ref[b] = pltpu.roll(band, offsets_ref[b], 1).astype(BF16)
    scalars.wait()
    for copy in copies[4:]:
        copy.wait()

    def pick(shard, row, n):
        return scalars_ref[shard, row, n].astype(jnp.int32)

    blocks = [(pick(shard, COUNT, 0) + UNROLL - 1) // UNROLL for shard in range(2)]

    def step(block, carry):
        shard = (block >= blocks[0]).astype(jnp.int32)
        first = (block - shard * blocks[0]) * UNROLL
        sums = []
        for u in range(UNROLL):
            n = first + u
            turns = radius_ref[...] * scalars_ref[shard, DEFOCUS, n]
            turns = turns - jnp.floor(turns + 0.5)
            t = 2.0 * turns + 0.1 / math.pi
            k = jnp.floor(t + 0.5)
            r = t - k
            z = r * r
            s = SINE[-1]
            for term in SINE[-2::-1]:
                s = s * z + term
            ctf = s * r * (1.0 - 2.0 * k * k)
            data = (ctf * pages_ref[shard, n].astype(F32)).astype(BF16)
            power = jnp.where(low, ctf * ctf, 0.0).astype(BF16)
            planes = jnp.concatenate([data, power], axis=1)
            poses = [pick(shard, POSES + j, n) for j in range(K_TOP)]
            rows = jnp.concatenate([placed_ref[b] for b in poses], axis=0)
            mixed = lax.dot_general(rows, planes, NN, preferred_element_type=F32)
            for j in range(K_TOP):
                m = mixed[j * half : (j + 1) * half] * scalars_ref[shard, WEIGHTS + j, n]
                pair = m[:, :LANES]
                stacked = jnp.concatenate(
                    [jnp.where(low, pair, 0.0), jnp.where(low, 0.0, pair), m[:, LANES:]], axis=0
                ).astype(BF16)
                cols = cols_ref[poses[j]]
                cols = jnp.concatenate([cols, cols], axis=0)
                spread = lax.dot_general(stacked, cols, NN, preferred_element_type=F32)
                c = pick(shard, CLASSES + j, n)
                sums.append((((c + up) % NEAR) * (n_class // NEAR) + c // NEAR, spread))
        for c, spread in sums:
            total_ref[c] += spread
        return carry

    lax.fori_loop(0, blocks[0] + blocks[1], step, 0)
    for d, out_ref in enumerate((out0_ref, out1_ref, out2_ref, out3_ref)):
        out_ref[...] = total_ref[pl.ds(d * (n_class // NEAR), n_class // NEAR)].astype(out_ref.dtype)


def insert_particles(place, offsets, row_kernel, col_kernel, pages, other_pages, n_class):
    n_pose, rows, _ = row_kernel.shape
    half = rows // 2
    out = (n_class, 3 * half, LCOLS)
    work = 2 * (pages.shape[0] - 1) * K_TOP * half * 2
    return pl.pallas_call(
        particle_kernel,
        out_shape=[jax.ShapeDtypeStruct((n_class // NEAR, *out[1:]), BF16)] * NEAR,
        in_specs=[pl.BlockSpec(memory_space=pltpu.SMEM)] + [pl.BlockSpec(memory_space=pl.ANY)] * 5,
        out_specs=[pl.BlockSpec(memory_space=pltpu.VMEM)] * NEAR,
        scratch_shapes=[
            pltpu.SMEM(offsets.shape, jnp.int32),
            pltpu.VMEM((n_pose, half, BAND), BF16),
            pltpu.VMEM(col_kernel.shape, BF16),
            pltpu.VMEM((2, pages.shape[0] - 1, *pages.shape[1:]), BF16),
            pltpu.VMEM((n_pose, half, LANES), BF16),
            pltpu.VMEM(out, F32),
            pltpu.VMEM((IROWS, LANES), F32),
            pltpu.VMEM((2, SMALL, LANES), BF16),
            pltpu.VMEM((2, SMALL, LANES), F32),
            pltpu.SMEM((2, SMALL, LANES), F32),
            pltpu.SemaphoreType.DMA((8,)),
        ],
        cost_estimate=pl.CostEstimate(
            flops=work * (IROWS * 2 * LANES + 3 * LANES * LCOLS) * 8,
            bytes_accessed=2 * 2 * math.prod(out),
            transcendentals=0,
        ),
        compiler_params=pltpu.CompilerParams(vmem_limit_bytes=ALL_VMEM),
        name="insert_particles",
    )(place, offsets, row_kernel, col_kernel, pages, other_pages)


def split_bf16(x):
    hi = x.astype(BF16)
    return hi, (x - hi.astype(F32)).astype(BF16)


def dot3(a, b, dims):
    (ah, al), (bh, bl) = a, b
    dot = functools.partial(lax.dot_general, dimension_numbers=dims, preferred_element_type=F32)
    return dot(ah, bh) + (dot(ah, bl) + dot(al, bh))


@functools.cache
def tables(groups):
    grid = np.arange(GRID)
    distance = np.minimum(grid, GRID - grid).astype(np.float64)
    blob = np.exp(-2.0 * np.pi**2 * blob_width**2 * distance**2 / GRID**2)
    angle = 2.0 * np.pi / GRID
    kernel = np.cos(angle * (grid[:, None] * grid[None, :] % GRID)) @ blob / GRID
    rows = np.arange(LROWS) - LROWS // 2
    cols = np.arange(LCOLS)
    factor = np.where(cols == 0, 1.0, 2.0)
    mix_rows = np.concatenate(
        [kernel[(rows[:, None] - rows[None, :]) % GRID], kernel[(rows[:, None] + rows[None, :]) % GRID]], axis=1
    )
    half = 0.5 * factor[:, None]
    mix_cols = np.concatenate(
        [half * kernel[(cols[:, None] - cols[None, :]) % GRID], half * kernel[(cols[:, None] + cols[None, :]) % GRID]],
        axis=1,
    )
    crop = np.arange(BOX) - BOX // 2
    correction = np.sinc(crop / GRID) ** 2
    row_angle = angle * (rows[:, None] * crop[None, :] % GRID)
    last_rows = np.concatenate([np.cos(row_angle), -np.sin(row_angle)], axis=0)
    last_rows = last_rows * (avg_scale / GRID) / correction[None, :]
    col_angle = angle * (crop[:, None] * cols[None, :] % GRID)
    last_cols = np.stack([np.cos(col_angle), np.sin(col_angle)], axis=0)
    last_cols = last_cols * factor[None, None, :] / correction[None, :, None]
    last_cols = last_cols.reshape(2, groups, BOX // groups, LCOLS).transpose(1, 0, 2, 3)
    last_cols = last_cols.reshape(groups, 2 * (BOX // groups), LCOLS)

    def two(x):
        x = x.astype(np.float32)
        hi = x.astype(jnp.bfloat16)
        lo = (x - hi.astype(np.float32)).astype(jnp.bfloat16)
        return np.stack([hi, lo])

    return two(mix_rows), two(mix_cols), two(last_rows), two(last_cols)


def refine_kernel(planes_ref, mix_rows_ref, mix_cols_ref, last_rows_ref, last_cols_ref, out_ref):
    blocks, third = planes_ref.shape[0], planes_ref.shape[1] // 3

    def plane(p):
        return jnp.concatenate([planes_ref[g, p * third : (p + 1) * third] for g in range(blocks)], axis=0).astype(F32)

    weight = plane(2)
    mix_rows = (mix_rows_ref[0], mix_rows_ref[1])
    mix_cols = (mix_cols_ref[0], mix_cols_ref[1])
    scale = jnp.ones_like(weight)
    for _ in range(ITERS):
        half = dot3(split_bf16(weight * scale), mix_cols, NN)
        half = jnp.concatenate([half[:, :LCOLS], half[:, LCOLS:]], axis=0)
        conv = dot3(mix_rows, split_bf16(half), NN)
        scale = scale / jnp.maximum(jnp.abs(conv), floor_value)
    last_cols = (last_cols_ref[0], last_cols_ref[1])
    real = dot3(last_cols, split_bf16(plane(0) * scale), NT)
    imag = dot3(last_cols, split_bf16(plane(1) * scale), NT)
    n = real.shape[0] // 2
    both = jnp.concatenate([real[:n] - imag[n:], real[n:] + imag[:n]], axis=1)
    out = dot3(split_bf16(both), (last_rows_ref[0], last_rows_ref[1]), NN)
    for i in range(out_ref.shape[0]):
        out_ref[i] = out.astype(out_ref.dtype)


def refine_class(planes, mix_rows, mix_cols, last_rows, last_cols, n_copies):
    vmem = pl.BlockSpec(memory_space=pltpu.VMEM)
    return pl.pallas_call(
        refine_kernel,
        out_shape=jax.ShapeDtypeStruct((n_copies, last_cols.shape[1] // 2, BOX), BF16),
        in_specs=[vmem] * 5,
        out_specs=vmem,
        cost_estimate=pl.CostEstimate(flops=2 * 10**9, bytes_accessed=3 * 10**6, transcendentals=0),
        compiler_params=pltpu.CompilerParams(vmem_limit_bytes=32 * 2**20),
        name="refine_class",
    )(planes, mix_rows, mix_cols, last_rows, last_cols)


def shift(value, axis, by):
    n = lax.axis_size(axis)
    return lax.ppermute(value, axis, [(i, (i + by) % n) for i in range(n)])


def neighbours(n, size):
    return [[first + i for i in range(size)] for first in range(0, n, size)]


def strided(n, stride):
    return [list(range(first, n, stride)) for first in range(stride)]


def added(parts):
    total = parts[0].astype(F32)
    for i in range(1, len(parts)):
        total = total + parts[i].astype(F32)
    return total


def sum_at_owner(parts, axis):
    n = lax.axis_size(axis)
    near = [parts[0], shift(parts[1], axis, 1), shift(parts[2], axis, 2), shift(parts[3], axis, -1)]
    here = added(near).astype(BF16)
    return added(lax.all_to_all(here, axis, 0, 0, axis_index_groups=strided(n, NEAR)))


def from_all(copies, axis):
    n = lax.axis_size(axis)
    far = lax.all_to_all(copies, axis, 0, 0, axis_index_groups=strided(n, NEAR))
    every = lax.all_to_all(
        jnp.broadcast_to(far, (NEAR, *far.shape)), axis, 0, 0, axis_index_groups=neighbours(n, NEAR)
    )
    return jnp.swapaxes(every, 0, 1).reshape(n, *copies.shape[1:])


def per_device(spectra, defocus, classes, poses, probs, counts, offsets, row_kernel, col_kernel):
    n_class = lax.axis_size("parts")
    group = lax.axis_size("sub") * lax.axis_size("pair")
    pages = prepare(counts, probs.T, defocus[None], classes.T, poses.T, spectra)
    other_pages = shift(pages, "pair", 1)
    place = jnp.stack([lax.axis_index("pair"), lax.axis_index("parts") % NEAR])
    col_rows = jnp.swapaxes(col_kernel, 1, 2)
    parts = insert_particles(place, offsets, row_kernel, col_rows, pages, other_pages, n_class)
    own = sum_at_owner(parts, "parts")
    planes = lax.all_gather(own, ("sub", "pair"), axis=0, tiled=False)
    mix_rows, mix_cols, last_rows, last_cols = tables(group)
    mine = lax.dynamic_index_in_dim(jnp.asarray(last_cols), lax.axis_index(("sub", "pair")), 1, keepdims=False)
    copies = refine_class(
        planes, jnp.asarray(mix_rows), jnp.asarray(mix_cols), jnp.asarray(last_rows), mine, n_class // NEAR
    )
    return from_all(copies, "parts").astype(F32)


def solution(mesh):
    shards = ("groups", "parts", "pair")
    placed = (
        P(shards, None, None),
        P(shards),
        P(shards, None),
        P(shards, None),
        P(shards, None),
        P(shards),
        P(),
        P(None, "sub", None),
        P(),
    )
    return jax.shard_map(
        per_device,
        mesh=mesh,
        in_specs=placed,
        out_specs=P("groups", ("sub", "pair"), None),
        check_vma=False,
    )
```

```python
import functools
import math

import jax
import jax.numpy as jnp
import numpy as np
from jax import lax
from jax.experimental import pallas as pl
from jax.experimental.pallas import tpu as pltpu
from jax.sharding import PartitionSpec as P

GRID = 512
BOX = 256
IROWS = 128
ICOLS = 64
LROWS = 256
LCOLS = 128
BAND = 64
K_TOP = 4
ITERS = 4
LANES = 128
UNROLL = 4
ALL_VMEM = 67043328
WEIGHTS, DEFOCUS, CLASSES, POSES, COUNT, SMALL = 0, K_TOP, K_TOP + 1, 2 * K_TOP + 1, 3 * K_TOP + 1, 16
NEAR = 4

blob_width = 1.5
avg_scale = 8.0
floor_value = 1.0

F32 = jnp.float32
BF16 = jnp.bfloat16
NT = (((1,), (1,)), ((), ()))
NN = (((1,), (0,)), ((), ()))


def sine_terms():
    r = np.cos(np.linspace(0.0, np.pi, 4001)) * 0.5
    r = r[np.abs(r) > 1e-3]
    z = r * r
    powers = np.stack([z**k for k in range(6)], axis=1)
    terms, *_ = np.linalg.lstsq(powers, np.sin(np.pi * r) / r, rcond=None)
    return [float(t) for t in terms]


SINE = sine_terms()


def start_all(pairs, sems):
    copies = [pltpu.make_async_copy(source, target, sems.at[i]) for i, (source, target) in enumerate(pairs)]
    for copy in copies:
        copy.start()
    return copies


def prepare_kernel(
    counts_in, probs_in, defocus_in, classes_in, poses_in, spec_in,
    pages_ref, counts_ref, probs_ref, defocus_ref, classes_ref, poses_ref, small_ref, sems,
):
    n_slots = spec_in.shape[0]
    copies = start_all(
        [
            (spec_in, pages_ref.at[pl.ds(0, n_slots)]),
            (counts_in, counts_ref),
            (probs_in, probs_ref),
            (defocus_in, defocus_ref),
            (classes_in, classes_ref),
            (poses_in, poses_ref),
        ],
        sems,
    )
    small_ref[...] = jnp.zeros_like(small_ref)
    pages_ref[n_slots] = jnp.zeros(pages_ref.shape[1:], BF16)
    for copy in copies[1:]:
        copy.wait()
    used = lax.broadcasted_iota(jnp.int32, (K_TOP, n_slots), 1) < counts_ref[0]
    small_ref[WEIGHTS : WEIGHTS + K_TOP, :n_slots] = jnp.where(used, probs_ref[...].astype(F32), 0.0)
    small_ref[DEFOCUS : DEFOCUS + 1, :n_slots] = defocus_ref[...].astype(F32)
    small_ref[CLASSES : CLASSES + K_TOP, :n_slots] = classes_ref[...].astype(F32)
    small_ref[POSES : POSES + K_TOP, :n_slots] = poses_ref[...].astype(F32)
    small_ref[COUNT : COUNT + 1, :] = jnp.full((1, LANES), counts_ref[0], jnp.int32).astype(F32)
    pages_ref[n_slots, :SMALL] = small_ref[...].astype(BF16)
    copies[0].wait()


def prepare(counts, probs, defocus, classes, poses, spectra):
    n_slots = spectra.shape[0]
    return pl.pallas_call(
        prepare_kernel,
        out_shape=jax.ShapeDtypeStruct((n_slots + 1, IROWS, LANES), BF16),
        in_specs=[pl.BlockSpec(memory_space=pl.ANY)] * 6,
        out_specs=pl.BlockSpec(memory_space=pltpu.VMEM),
        scratch_shapes=[
            pltpu.SMEM(counts.shape, jnp.int32),
            pltpu.VMEM(probs.shape, BF16),
            pltpu.VMEM(defocus.shape, BF16),
            pltpu.VMEM(classes.shape, jnp.int32),
            pltpu.VMEM(poses.shape, jnp.int32),
            pltpu.VMEM((SMALL, LANES), F32),
            pltpu.SemaphoreType.DMA((6,)),
        ],
        cost_estimate=pl.CostEstimate(flops=10**6, bytes_accessed=2 * 10**6, transcendentals=0),
        compiler_params=pltpu.CompilerParams(vmem_limit_bytes=ALL_VMEM),
        name="prepare",
    )(counts, probs, defocus, classes, poses, spectra)


def particle_kernel(
    place_ref, offsets_in, rk_in, ck_in, own_in, other_in,
    out0_ref, out1_ref, out2_ref, out3_ref,
    offsets_ref, rows_ref, cols_ref, pages_ref, placed_ref, total_ref, radius_ref, page_ref, small_ref, scalars_ref, sems,
):
    n_slots = pages_ref.shape[1]
    n_class = total_ref.shape[0]
    n_pose, half = placed_ref.shape[0], placed_ref.shape[1]
    first_row = pl.multiple_of(place_ref[0] * half, half)
    here = place_ref[1]
    copies = start_all(
        [
            (own_in.at[n_slots, pl.ds(0, SMALL)], page_ref.at[0]),
            (other_in.at[n_slots, pl.ds(0, SMALL)], page_ref.at[1]),
            (offsets_in, offsets_ref),
            (rk_in.at[:, pl.ds(first_row, half), :], rows_ref),
            (own_in.at[pl.ds(0, n_slots)], pages_ref.at[0]),
            (ck_in, cols_ref),
            (other_in.at[pl.ds(0, n_slots)], pages_ref.at[1]),
        ],
        sems,
    )
    lane = lax.broadcasted_iota(jnp.int32, (1, LANES), 1)
    low = lane < ICOLS
    row_freq = (lax.broadcasted_iota(jnp.int32, (IROWS, LANES), 0) - IROWS // 2).astype(F32)
    col_freq = (lax.broadcasted_iota(jnp.int32, (IROWS, LANES), 1) & (ICOLS - 1)).astype(F32)
    radius_ref[...] = (row_freq * row_freq + col_freq * col_freq) * (10.0 / (ICOLS * ICOLS))
    total_ref[...] = jnp.zeros_like(total_ref)
    copies[0].wait()
    copies[1].wait()
    small_ref[...] = page_ref[...].astype(F32)
    scalars = pltpu.make_async_copy(small_ref, scalars_ref, sems.at[7])
    scalars.start()
    copies[2].wait()
    copies[3].wait()
    for b in range(n_pose):
        band = rows_ref[b].astype(F32)
        band = jnp.concatenate([band, jnp.zeros((half, LANES - BAND), F32)], axis=1)
        placed_ref[b] = pltpu.roll(band, offsets_ref[b], 1).astype(BF16)
    scalars.wait()
    for copy in copies[4:]:
        copy.wait()

    def pick(shard, row, n):
        return scalars_ref[shard, row, n].astype(jnp.int32)

    blocks = [(pick(shard, COUNT, 0) + UNROLL - 1) // UNROLL for shard in range(2)]

    def step(block, carry):
        shard = (block >= blocks[0]).astype(jnp.int32)
        first = (block - shard * blocks[0]) * UNROLL
        sums = []
        for u in range(UNROLL):
            n = first + u
            turns = radius_ref[...] * scalars_ref[shard, DEFOCUS, n]
            turns = turns - jnp.floor(turns + 0.5)
            t = 2.0 * turns + 0.1 / math.pi
            k = jnp.floor(t + 0.5)
            r = t - k
            z = r * r
            s = SINE[-1]
            for term in SINE[-2::-1]:
                s = s * z + term
            ctf = s * r * (1.0 - 2.0 * k * k)
            data = (ctf * pages_ref[shard, n].astype(F32)).astype(BF16)
            power = jnp.where(low, ctf * ctf, 0.0).astype(BF16)
            planes = jnp.concatenate([data, power], axis=1)
            poses = [pick(shard, POSES + j, n) for j in range(K_TOP)]
            rows = jnp.concatenate([placed_ref[b] for b in poses], axis=0)
            mixed = lax.dot_general(rows, planes, NN, preferred_element_type=F32)
            for j in range(K_TOP):
                m = mixed[j * half : (j + 1) * half] * scalars_ref[shard, WEIGHTS + j, n]
                pair = m[:, :LANES]
                stacked = jnp.concatenate(
                    [jnp.where(low, pair, 0.0), jnp.where(low, 0.0, pair), m[:, LANES:]], axis=0
                ).astype(BF16)
                cols = cols_ref[poses[j]]
                cols = jnp.concatenate([cols, cols], axis=0)
                spread = lax.dot_general(stacked, cols, NN, preferred_element_type=F32)
                c = pick(shard, CLASSES + j, n)
                d = (c + n_class - here) % NEAR
                collector = here + jnp.where(d == NEAR - 1, -1, d)
                far = ((c + 2 * n_class - collector) % n_class) // NEAR
                sums.append((d * (n_class // NEAR) + far, spread))
        for c, spread in sums:
            total_ref[c] += spread
        return carry

    lax.fori_loop(0, blocks[0] + blocks[1], step, 0)
    for d, out_ref in enumerate((out0_ref, out1_ref, out2_ref, out3_ref)):
        out_ref[...] = total_ref[pl.ds(d * (n_class // NEAR), n_class // NEAR)].astype(out_ref.dtype)


def insert_particles(place, offsets, row_kernel, col_kernel, pages, other_pages, n_class):
    n_pose, rows, _ = row_kernel.shape
    half = rows // 2
    out = (n_class, 3 * half, LCOLS)
    work = 2 * (pages.shape[0] - 1) * K_TOP * half * 2
    return pl.pallas_call(
        particle_kernel,
        out_shape=[jax.ShapeDtypeStruct((n_class // NEAR, *out[1:]), BF16)] * NEAR,
        in_specs=[pl.BlockSpec(memory_space=pltpu.SMEM)] + [pl.BlockSpec(memory_space=pl.ANY)] * 5,
        out_specs=[pl.BlockSpec(memory_space=pltpu.VMEM)] * NEAR,
        scratch_shapes=[
            pltpu.SMEM(offsets.shape, jnp.int32),
            pltpu.VMEM((n_pose, half, BAND), BF16),
            pltpu.VMEM(col_kernel.shape, BF16),
            pltpu.VMEM((2, pages.shape[0] - 1, *pages.shape[1:]), BF16),
            pltpu.VMEM((n_pose, half, LANES), BF16),
            pltpu.VMEM(out, F32),
            pltpu.VMEM((IROWS, LANES), F32),
            pltpu.VMEM((2, SMALL, LANES), BF16),
            pltpu.VMEM((2, SMALL, LANES), F32),
            pltpu.SMEM((2, SMALL, LANES), F32),
            pltpu.SemaphoreType.DMA((8,)),
        ],
        cost_estimate=pl.CostEstimate(
            flops=work * (IROWS * 2 * LANES + 3 * LANES * LCOLS) * 8,
            bytes_accessed=2 * 2 * math.prod(out),
            transcendentals=0,
        ),
        compiler_params=pltpu.CompilerParams(vmem_limit_bytes=ALL_VMEM),
        name="insert_particles",
    )(place, offsets, row_kernel, col_kernel, pages, other_pages)


def split_bf16(x):
    hi = x.astype(BF16)
    return hi, (x - hi.astype(F32)).astype(BF16)


def dot3(a, b, dims):
    (ah, al), (bh, bl) = a, b
    dot = functools.partial(lax.dot_general, dimension_numbers=dims, preferred_element_type=F32)
    return dot(ah, bh) + (dot(ah, bl) + dot(al, bh))


@functools.cache
def tables(groups):
    grid = np.arange(GRID)
    distance = np.minimum(grid, GRID - grid).astype(np.float64)
    blob = np.exp(-2.0 * np.pi**2 * blob_width**2 * distance**2 / GRID**2)
    angle = 2.0 * np.pi / GRID
    kernel = np.cos(angle * (grid[:, None] * grid[None, :] % GRID)) @ blob / GRID
    rows = np.arange(LROWS) - LROWS // 2
    cols = np.arange(LCOLS)
    factor = np.where(cols == 0, 1.0, 2.0)
    mix_rows = np.concatenate(
        [kernel[(rows[:, None] - rows[None, :]) % GRID], kernel[(rows[:, None] + rows[None, :]) % GRID]], axis=1
    )
    half = 0.5 * factor[:, None]
    mix_cols = np.concatenate(
        [half * kernel[(cols[:, None] - cols[None, :]) % GRID], half * kernel[(cols[:, None] + cols[None, :]) % GRID]],
        axis=1,
    )
    crop = np.arange(BOX) - BOX // 2
    correction = np.sinc(crop / GRID) ** 2
    row_angle = angle * (rows[:, None] * crop[None, :] % GRID)
    last_rows = np.concatenate([np.cos(row_angle), -np.sin(row_angle)], axis=0)
    last_rows = last_rows * (avg_scale / GRID) / correction[None, :]
    col_angle = angle * (crop[:, None] * cols[None, :] % GRID)
    last_cols = np.stack([np.cos(col_angle), np.sin(col_angle)], axis=0)
    last_cols = last_cols * factor[None, None, :] / correction[None, :, None]
    last_cols = last_cols.reshape(2, groups, BOX // groups, LCOLS).transpose(1, 0, 2, 3)
    last_cols = last_cols.reshape(groups, 2 * (BOX // groups), LCOLS)

    def two(x):
        x = x.astype(np.float32)
        hi = x.astype(jnp.bfloat16)
        lo = (x - hi.astype(np.float32)).astype(jnp.bfloat16)
        return np.stack([hi, lo])

    return two(mix_rows), two(mix_cols), two(last_rows), two(last_cols)


def refine_kernel(planes_ref, mix_rows_ref, mix_cols_ref, last_rows_ref, last_cols_ref, out_ref):
    blocks, third = planes_ref.shape[0], planes_ref.shape[1] // 3

    def plane(p):
        return jnp.concatenate([planes_ref[g, p * third : (p + 1) * third] for g in range(blocks)], axis=0).astype(F32)

    weight = plane(2)
    mix_rows = (mix_rows_ref[0], mix_rows_ref[1])
    mix_cols = (mix_cols_ref[0], mix_cols_ref[1])
    scale = jnp.ones_like(weight)
    for _ in range(ITERS):
        half = dot3(split_bf16(weight * scale), mix_cols, NN)
        half = jnp.concatenate([half[:, :LCOLS], half[:, LCOLS:]], axis=0)
        conv = dot3(mix_rows, split_bf16(half), NN)
        scale = scale / jnp.maximum(jnp.abs(conv), floor_value)
    last_cols = (last_cols_ref[0], last_cols_ref[1])
    real = dot3(last_cols, split_bf16(plane(0) * scale), NT)
    imag = dot3(last_cols, split_bf16(plane(1) * scale), NT)
    n = real.shape[0] // 2
    both = jnp.concatenate([real[:n] - imag[n:], real[n:] + imag[:n]], axis=1)
    out = dot3(split_bf16(both), (last_rows_ref[0], last_rows_ref[1]), NN)
    out_ref[...] = out.astype(out_ref.dtype)


def refine_class(planes, mix_rows, mix_cols, last_rows, last_cols):
    vmem = pl.BlockSpec(memory_space=pltpu.VMEM)
    return pl.pallas_call(
        refine_kernel,
        out_shape=jax.ShapeDtypeStruct((last_cols.shape[1] // 2, BOX), BF16),
        in_specs=[vmem] * 5,
        out_specs=vmem,
        cost_estimate=pl.CostEstimate(flops=2 * 10**9, bytes_accessed=3 * 10**6, transcendentals=0),
        compiler_params=pltpu.CompilerParams(vmem_limit_bytes=32 * 2**20),
        name="refine_class",
    )(planes, mix_rows, mix_cols, last_rows, last_cols)


def shift(value, axis, by):
    n = lax.axis_size(axis)
    return lax.ppermute(value, axis, [(i, (i + by) % n) for i in range(n)])


def collect_kernel(a_ref, b_ref, c_ref, d_ref, *outs):
    for i, out_ref in enumerate(outs):
        total = a_ref[i].astype(F32) + b_ref[i].astype(F32) + c_ref[i].astype(F32) + d_ref[i].astype(F32)
        out_ref[...] = total.astype(out_ref.dtype)


def own_kernel(own_ref, *refs):
    total = own_ref[...]
    for ref in refs[:-1]:
        total = total + ref[...].astype(F32)
    for i in range(refs[-1].shape[0]):
        refs[-1][i] = total


def whole_arrays(kernel, outs, *operands):
    vmem = pl.BlockSpec(memory_space=pltpu.VMEM)
    return pl.pallas_call(
        kernel,
        out_shape=outs,
        in_specs=[vmem] * len(operands),
        out_specs=jax.tree.map(lambda _: vmem, outs),
        cost_estimate=pl.CostEstimate(flops=10**6, bytes_accessed=10**6, transcendentals=0),
        compiler_params=pltpu.CompilerParams(vmem_limit_bytes=8 * 2**20),
        name=kernel.__name__,
    )(*operands)


def far_first(n):
    return sorted(range(1, n), key=lambda i: -min(i, n - i))


def sum_at_owner(parts, axis, n_copies):
    n_far = lax.axis_size(axis) // NEAR
    near = [parts[0], shift(parts[1], axis, 1), shift(parts[2], axis, 2), shift(parts[3], axis, -1)]
    shape = parts[0].shape[1:]
    outs = [jax.ShapeDtypeStruct(shape, F32)] + [jax.ShapeDtypeStruct(shape, BF16)] * (n_far - 1)
    sums = whole_arrays(collect_kernel, outs, *near)
    far = [shift(sums[i], axis, NEAR * i) for i in far_first(n_far)]
    return whole_arrays(own_kernel, jax.ShapeDtypeStruct((n_copies, *shape), F32), sums[0], *far)


def row_kernel(*refs):
    for i, ref in enumerate(refs[:-1]):
        refs[-1][i] = ref[...]


def place_kernel(place_ref, own_ref, *refs):
    out_ref = refs[-1]
    n_class = out_ref.shape[0]
    n_far = own_ref.shape[0]
    for ref, d in zip((own_ref, *refs[:-1]), (0, 1, 2, -1)):
        for i in range(n_far):
            out_ref[(place_ref[1] + d + n_class - NEAR * i) % n_class] = ref[i].astype(F32)


def from_all(value, axis, place):
    n = lax.axis_size(axis)
    n_far = n // NEAR
    far = {0: value}
    for i in far_first(n_far):
        far[i] = shift(value, axis, NEAR * i)
    row = [far[i] for i in range(n_far)]
    own = whole_arrays(row_kernel, jax.ShapeDtypeStruct((n_far, *value.shape), BF16), *row)
    near = [shift(own, axis, -1), shift(own, axis, -2), shift(own, axis, 1)]
    vmem = pl.BlockSpec(memory_space=pltpu.VMEM)
    return pl.pallas_call(
        place_kernel,
        out_shape=jax.ShapeDtypeStruct((n, *value.shape), F32),
        in_specs=[pl.BlockSpec(memory_space=pltpu.SMEM)] + [vmem] * NEAR,
        out_specs=vmem,
        cost_estimate=pl.CostEstimate(flops=10**6, bytes_accessed=2 * 10**6, transcendentals=0),
        compiler_params=pltpu.CompilerParams(vmem_limit_bytes=16 * 2**20),
        name="place_averages",
    )(place, own, *near)


def per_device(spectra, defocus, classes, poses, probs, counts, offsets, row_kernel, col_kernel):
    n_class = lax.axis_size("parts")
    group = lax.axis_size("sub") * lax.axis_size("pair")
    pages = prepare(counts, probs.T, defocus[None], classes.T, poses.T, spectra)
    other_pages = shift(pages, "pair", 1)
    place = jnp.stack([lax.axis_index("pair"), lax.axis_index("parts")])
    col_rows = jnp.swapaxes(col_kernel, 1, 2)
    parts = insert_particles(place, offsets, row_kernel, col_rows, pages, other_pages, n_class)
    planes = lax.all_to_all(sum_at_owner(parts, "parts", group), ("sub", "pair"), 0, 0, tiled=True)
    mix_rows, mix_cols, last_rows, last_cols = tables(group)
    mine = lax.dynamic_index_in_dim(jnp.asarray(last_cols), lax.axis_index(("sub", "pair")), 1, keepdims=False)
    average = refine_class(planes, jnp.asarray(mix_rows), jnp.asarray(mix_cols), jnp.asarray(last_rows), mine)
    return from_all(average, "parts", place)


def solution(mesh):
    shards = ("groups", "parts", "pair")
    placed = (
        P(shards, None, None),
        P(shards),
        P(shards, None),
        P(shards, None),
        P(shards, None),
        P(shards),
        P(),
        P(None, "sub", None),
        P(),
    )
    return jax.shard_map(
        per_device,
        mesh=mesh,
        in_specs=placed,
        out_specs=P("groups", ("sub", "pair"), None),
        check_vma=False,
    )
```

```python
import functools
import math

import jax
import jax.numpy as jnp
import numpy as np
from jax import lax
from jax.experimental import pallas as pl
from jax.experimental.pallas import tpu as pltpu
from jax.sharding import PartitionSpec as P

GRID = 512
BOX = 256
IROWS = 128
ICOLS = 64
LROWS = 256
LCOLS = 128
BAND = 64
K_TOP = 4
ITERS = 4
LANES = 128
UNROLL = 4
ALL_VMEM = 67043328
WEIGHTS, DEFOCUS, CLASSES, POSES, COUNT, SMALL = 0, K_TOP, K_TOP + 1, 2 * K_TOP + 1, 3 * K_TOP + 1, 16
NEAR = 4

blob_width = 1.5
avg_scale = 8.0
floor_value = 1.0

F32 = jnp.float32
BF16 = jnp.bfloat16
NT = (((1,), (1,)), ((), ()))
NN = (((1,), (0,)), ((), ()))


def sine_terms():
    r = np.cos(np.linspace(0.0, np.pi, 4001)) * 0.5
    r = r[np.abs(r) > 1e-3]
    z = r * r
    powers = np.stack([z**k for k in range(6)], axis=1)
    terms, *_ = np.linalg.lstsq(powers, np.sin(np.pi * r) / r, rcond=None)
    return [float(t) for t in terms]


SINE = sine_terms()


def start_all(pairs, sems):
    copies = [pltpu.make_async_copy(source, target, sems.at[i]) for i, (source, target) in enumerate(pairs)]
    for copy in copies:
        copy.start()
    return copies


def prepare_kernel(
    counts_in, probs_in, defocus_in, classes_in, poses_in, spec_in,
    pages_ref, counts_ref, probs_ref, defocus_ref, classes_ref, poses_ref, small_ref, sems,
):
    n_slots = spec_in.shape[0]
    copies = start_all(
        [
            (spec_in, pages_ref.at[pl.ds(0, n_slots)]),
            (counts_in, counts_ref),
            (probs_in, probs_ref),
            (defocus_in, defocus_ref),
            (classes_in, classes_ref),
            (poses_in, poses_ref),
        ],
        sems,
    )
    small_ref[...] = jnp.zeros_like(small_ref)
    pages_ref[n_slots] = jnp.zeros(pages_ref.shape[1:], BF16)
    for copy in copies[1:]:
        copy.wait()
    used = lax.broadcasted_iota(jnp.int32, (K_TOP, n_slots), 1) < counts_ref[0]
    small_ref[WEIGHTS : WEIGHTS + K_TOP, :n_slots] = jnp.where(used, probs_ref[...].astype(F32), 0.0)
    small_ref[DEFOCUS : DEFOCUS + 1, :n_slots] = defocus_ref[...].astype(F32)
    small_ref[CLASSES : CLASSES + K_TOP, :n_slots] = classes_ref[...].astype(F32)
    small_ref[POSES : POSES + K_TOP, :n_slots] = poses_ref[...].astype(F32)
    small_ref[COUNT : COUNT + 1, :] = jnp.full((1, LANES), counts_ref[0], jnp.int32).astype(F32)
    pages_ref[n_slots, :SMALL] = small_ref[...].astype(BF16)
    copies[0].wait()


def prepare(counts, probs, defocus, classes, poses, spectra):
    n_slots = spectra.shape[0]
    return pl.pallas_call(
        prepare_kernel,
        out_shape=jax.ShapeDtypeStruct((n_slots + 1, IROWS, LANES), BF16),
        in_specs=[pl.BlockSpec(memory_space=pl.ANY)] * 6,
        out_specs=pl.BlockSpec(memory_space=pltpu.VMEM),
        scratch_shapes=[
            pltpu.SMEM(counts.shape, jnp.int32),
            pltpu.VMEM(probs.shape, BF16),
            pltpu.VMEM(defocus.shape, BF16),
            pltpu.VMEM(classes.shape, jnp.int32),
            pltpu.VMEM(poses.shape, jnp.int32),
            pltpu.VMEM((SMALL, LANES), F32),
            pltpu.SemaphoreType.DMA((6,)),
        ],
        cost_estimate=pl.CostEstimate(flops=10**6, bytes_accessed=2 * 10**6, transcendentals=0),
        compiler_params=pltpu.CompilerParams(vmem_limit_bytes=ALL_VMEM),
        name="prepare",
    )(counts, probs, defocus, classes, poses, spectra)


def particle_kernel(
    place_ref, offsets_in, rk_in, ck_in, own_in, other_in,
    out0_ref, out1_ref, out2_ref, out3_ref,
    offsets_ref, rows_ref, cols_ref, pages_ref, placed_ref, total_ref, radius_ref, page_ref, small_ref, scalars_ref, sems,
):
    n_slots = pages_ref.shape[1]
    n_class = total_ref.shape[0]
    n_pose, half = placed_ref.shape[0], placed_ref.shape[1]
    first_row = pl.multiple_of(place_ref[0] * half, half)
    here = place_ref[1]
    copies = start_all(
        [
            (own_in.at[n_slots, pl.ds(0, SMALL)], page_ref.at[0]),
            (other_in.at[n_slots, pl.ds(0, SMALL)], page_ref.at[1]),
            (offsets_in, offsets_ref),
            (rk_in.at[:, pl.ds(first_row, half), :], rows_ref),
            (own_in.at[pl.ds(0, n_slots)], pages_ref.at[0]),
            (ck_in, cols_ref),
            (other_in.at[pl.ds(0, n_slots)], pages_ref.at[1]),
        ],
        sems,
    )
    lane = lax.broadcasted_iota(jnp.int32, (1, LANES), 1)
    low = lane < ICOLS
    packed = (IROWS // 2, LANES)
    row_freq = lax.broadcasted_iota(jnp.int32, packed, 0) - jnp.where(low, IROWS // 2, 0)
    row_freq = row_freq.astype(F32)
    col_freq = (lax.broadcasted_iota(jnp.int32, packed, 1) & (ICOLS - 1)).astype(F32)
    radius_ref[...] = (row_freq * row_freq + col_freq * col_freq) * (10.0 / (ICOLS * ICOLS))
    total_ref[...] = jnp.zeros_like(total_ref)
    copies[0].wait()
    copies[1].wait()
    small_ref[...] = page_ref[...].astype(F32)
    scalars = pltpu.make_async_copy(small_ref, scalars_ref, sems.at[7])
    scalars.start()
    copies[2].wait()
    copies[3].wait()
    for b in range(n_pose):
        band = rows_ref[b].astype(F32)
        band = jnp.concatenate([band, jnp.zeros((half, LANES - BAND), F32)], axis=1)
        placed_ref[b] = pltpu.roll(band, offsets_ref[b], 1).astype(BF16)
    scalars.wait()
    for copy in copies[4:]:
        copy.wait()

    def pick(shard, row, n):
        return scalars_ref[shard, row, n].astype(jnp.int32)

    blocks = [(pick(shard, COUNT, 0) + UNROLL - 1) // UNROLL for shard in range(2)]

    def step(block, carry):
        shard = (block >= blocks[0]).astype(jnp.int32)
        first = (block - shard * blocks[0]) * UNROLL
        sums = []
        for u in range(UNROLL):
            n = first + u
            turns = radius_ref[...] * scalars_ref[shard, DEFOCUS, n]
            turns = turns - jnp.floor(turns + 0.5)
            t = 2.0 * turns + 0.1 / math.pi
            k = jnp.floor(t + 0.5)
            r = t - k
            z = r * r
            s = SINE[-1]
            for term in SINE[-2::-1]:
                s = s * z + term
            ctf = s * r * (1.0 - 2.0 * k * k)
            turned = pltpu.roll(ctf, ICOLS, 1)
            ctf = jnp.concatenate([jnp.where(low, ctf, turned), jnp.where(low, turned, ctf)], axis=0)
            data = (ctf * pages_ref[shard, n].astype(F32)).astype(BF16)
            power = jnp.where(low, ctf * ctf, 0.0).astype(BF16)
            planes = jnp.concatenate([data, power], axis=1)
            poses = [pick(shard, POSES + j, n) for j in range(K_TOP)]
            rows = jnp.concatenate([placed_ref[b] for b in poses], axis=0)
            mixed = lax.dot_general(rows, planes, NN, preferred_element_type=F32)
            for j in range(K_TOP):
                m = mixed[j * half : (j + 1) * half] * scalars_ref[shard, WEIGHTS + j, n]
                pair = m[:, :LANES]
                stacked = jnp.concatenate(
                    [jnp.where(low, pair, 0.0), jnp.where(low, 0.0, pair), m[:, LANES:]], axis=0
                ).astype(BF16)
                cols = cols_ref[poses[j]]
                cols = jnp.concatenate([cols, cols], axis=0)
                spread = lax.dot_general(stacked, cols, NN, preferred_element_type=F32)
                c = pick(shard, CLASSES + j, n)
                d = (c + n_class - here) % NEAR
                sums.append((d * (n_class // NEAR) + c // NEAR, spread))
        for c, spread in sums:
            total_ref[c] += spread
        return carry

    lax.fori_loop(0, blocks[0] + blocks[1], step, 0)
    for d, out_ref in enumerate((out0_ref, out1_ref, out2_ref, out3_ref)):
        out_ref[...] = total_ref[pl.ds(d * (n_class // NEAR), n_class // NEAR)].astype(out_ref.dtype)


def insert_particles(place, offsets, row_kernel, col_kernel, pages, other_pages, n_class):
    n_pose, rows, _ = row_kernel.shape
    half = rows // 2
    out = (n_class, 3 * half, LCOLS)
    work = 2 * (pages.shape[0] - 1) * K_TOP * half * 2
    return pl.pallas_call(
        particle_kernel,
        out_shape=[jax.ShapeDtypeStruct((n_class // NEAR, *out[1:]), BF16)] * NEAR,
        in_specs=[pl.BlockSpec(memory_space=pltpu.SMEM)] + [pl.BlockSpec(memory_space=pl.ANY)] * 5,
        out_specs=[pl.BlockSpec(memory_space=pltpu.VMEM)] * NEAR,
        scratch_shapes=[
            pltpu.SMEM(offsets.shape, jnp.int32),
            pltpu.VMEM((n_pose, half, BAND), BF16),
            pltpu.VMEM(col_kernel.shape, BF16),
            pltpu.VMEM((2, pages.shape[0] - 1, *pages.shape[1:]), BF16),
            pltpu.VMEM((n_pose, half, LANES), BF16),
            pltpu.VMEM(out, F32),
            pltpu.VMEM((IROWS // 2, LANES), F32),
            pltpu.VMEM((2, SMALL, LANES), BF16),
            pltpu.VMEM((2, SMALL, LANES), F32),
            pltpu.SMEM((2, SMALL, LANES), F32),
            pltpu.SemaphoreType.DMA((8,)),
        ],
        cost_estimate=pl.CostEstimate(
            flops=work * (IROWS * 2 * LANES + 3 * LANES * LCOLS) * 8,
            bytes_accessed=2 * 2 * math.prod(out),
            transcendentals=0,
        ),
        compiler_params=pltpu.CompilerParams(vmem_limit_bytes=ALL_VMEM),
        name="insert_particles",
    )(place, offsets, row_kernel, col_kernel, pages, other_pages)


def split_bf16(x):
    hi = x.astype(BF16)
    return hi, (x - hi.astype(F32)).astype(BF16)


def dot3(a, b, dims):
    (ah, al), (bh, bl) = a, b
    dot = functools.partial(lax.dot_general, dimension_numbers=dims, preferred_element_type=F32)
    return dot(ah, bh) + (dot(ah, bl) + dot(al, bh))


@functools.cache
def tables(groups):
    grid = np.arange(GRID)
    distance = np.minimum(grid, GRID - grid).astype(np.float64)
    blob = np.exp(-2.0 * np.pi**2 * blob_width**2 * distance**2 / GRID**2)
    angle = 2.0 * np.pi / GRID
    kernel = np.cos(angle * (grid[:, None] * grid[None, :] % GRID)) @ blob / GRID
    rows = np.arange(LROWS) - LROWS // 2
    cols = np.arange(LCOLS)
    factor = np.where(cols == 0, 1.0, 2.0)
    mix_rows = np.concatenate(
        [kernel[(rows[:, None] - rows[None, :]) % GRID], kernel[(rows[:, None] + rows[None, :]) % GRID]], axis=1
    )
    half = 0.5 * factor[:, None]
    mix_cols = np.concatenate(
        [half * kernel[(cols[:, None] - cols[None, :]) % GRID], half * kernel[(cols[:, None] + cols[None, :]) % GRID]],
        axis=1,
    )
    crop = np.arange(BOX) - BOX // 2
    correction = np.sinc(crop / GRID) ** 2
    row_angle = angle * (rows[:, None] * crop[None, :] % GRID)
    last_rows = np.concatenate([np.cos(row_angle), -np.sin(row_angle)], axis=0)
    last_rows = last_rows * (avg_scale / GRID) / correction[None, :]
    col_angle = angle * (crop[:, None] * cols[None, :] % GRID)
    last_cols = np.stack([np.cos(col_angle), np.sin(col_angle)], axis=0)
    last_cols = last_cols * factor[None, None, :] / correction[None, :, None]
    last_cols = last_cols.reshape(2, groups, BOX // groups, LCOLS).transpose(1, 0, 2, 3)
    last_cols = last_cols.reshape(groups, 2 * (BOX // groups), LCOLS)

    def two(x):
        x = x.astype(np.float32)
        hi = x.astype(jnp.bfloat16)
        lo = (x - hi.astype(np.float32)).astype(jnp.bfloat16)
        return np.stack([hi, lo])

    return two(mix_rows), two(mix_cols), two(last_rows), two(last_cols)


def refine_kernel(planes_ref, mix_rows_ref, mix_cols_ref, last_rows_ref, last_cols_ref, out_ref):
    blocks, third = planes_ref.shape[0], planes_ref.shape[1] // 3

    def plane(p):
        return jnp.concatenate([planes_ref[g, p * third : (p + 1) * third] for g in range(blocks)], axis=0).astype(F32)

    weight = plane(2)
    mix_rows = (mix_rows_ref[0], mix_rows_ref[1])
    mix_cols = (mix_cols_ref[0], mix_cols_ref[1])
    scale = jnp.ones_like(weight)
    for _ in range(ITERS):
        half = dot3(split_bf16(weight * scale), mix_cols, NN)
        half = jnp.concatenate([half[:, :LCOLS], half[:, LCOLS:]], axis=0)
        conv = dot3(mix_rows, split_bf16(half), NN)
        scale = scale / jnp.maximum(jnp.abs(conv), floor_value)
    last_cols = (last_cols_ref[0], last_cols_ref[1])
    real = dot3(last_cols, split_bf16(plane(0) * scale), NT)
    imag = dot3(last_cols, split_bf16(plane(1) * scale), NT)
    n = real.shape[0] // 2
    both = jnp.concatenate([real[:n] - imag[n:], real[n:] + imag[:n]], axis=1)
    out = dot3(split_bf16(both), (last_rows_ref[0], last_rows_ref[1]), NN)
    for i in range(out_ref.shape[0]):
        out_ref[i] = out.astype(out_ref.dtype)


def refine_class(planes, mix_rows, mix_cols, last_rows, last_cols, n_copies):
    vmem = pl.BlockSpec(memory_space=pltpu.VMEM)
    return pl.pallas_call(
        refine_kernel,
        out_shape=jax.ShapeDtypeStruct((n_copies, last_cols.shape[1] // 2, BOX), BF16),
        in_specs=[vmem] * 5,
        out_specs=vmem,
        cost_estimate=pl.CostEstimate(flops=2 * 10**9, bytes_accessed=3 * 10**6, transcendentals=0),
        compiler_params=pltpu.CompilerParams(vmem_limit_bytes=32 * 2**20),
        name="refine_class",
    )(planes, mix_rows, mix_cols, last_rows, last_cols)


def shift(value, axis, by):
    n = lax.axis_size(axis)
    return lax.ppermute(value, axis, [(i, (i + by) % n) for i in range(n)])


def strided(n, stride):
    return [list(range(first, n, stride)) for first in range(stride)]


def added(parts):
    total = parts[0].astype(F32)
    for i in range(1, len(parts)):
        total = total + parts[i].astype(F32)
    return total


def collect_kernel(a_ref, b_ref, c_ref, d_ref, out_ref):
    out_ref[...] = added([a_ref[...], b_ref[...], c_ref[...], d_ref[...]]).astype(out_ref.dtype)


def collect(parts):
    vmem = pl.BlockSpec(memory_space=pltpu.VMEM)
    return pl.pallas_call(
        collect_kernel,
        out_shape=jax.ShapeDtypeStruct(parts[0].shape, BF16),
        in_specs=[vmem] * NEAR,
        out_specs=vmem,
        cost_estimate=pl.CostEstimate(flops=10**6, bytes_accessed=10**6, transcendentals=0),
        compiler_params=pltpu.CompilerParams(vmem_limit_bytes=8 * 2**20),
        name="collect",
    )(*parts)


def sum_at_owner(parts, axis):
    here = collect([parts[0], shift(parts[1], axis, 1), shift(parts[2], axis, 2), shift(parts[3], axis, -1)])
    return added(lax.all_to_all(here, axis, 0, 0, axis_index_groups=strided(lax.axis_size(axis), NEAR)))


def place_kernel(place_ref, own_ref, *refs):
    out_ref = refs[-1]
    n_class = out_ref.shape[0]
    for ref, d in zip((own_ref, *refs[:-1]), (0, 1, 2, -1)):
        first = (place_ref[1] + d + n_class) % NEAR
        for i in range(own_ref.shape[0]):
            out_ref[NEAR * i + first] = ref[i].astype(F32)


def from_all(copies, axis, place):
    n = lax.axis_size(axis)
    own = lax.all_to_all(copies, axis, 0, 0, axis_index_groups=strided(n, NEAR))
    near = [shift(own, axis, -1), shift(own, axis, -2), shift(own, axis, 1)]
    vmem = pl.BlockSpec(memory_space=pltpu.VMEM)
    return pl.pallas_call(
        place_kernel,
        out_shape=jax.ShapeDtypeStruct((n, *copies.shape[1:]), F32),
        in_specs=[pl.BlockSpec(memory_space=pltpu.SMEM)] + [vmem] * NEAR,
        out_specs=vmem,
        cost_estimate=pl.CostEstimate(flops=10**6, bytes_accessed=2 * 10**6, transcendentals=0),
        compiler_params=pltpu.CompilerParams(vmem_limit_bytes=16 * 2**20),
        name="place_averages",
    )(place, own, *near)


def per_device(spectra, defocus, classes, poses, probs, counts, offsets, row_kernel, col_kernel):
    n_class = lax.axis_size("parts")
    group = lax.axis_size("sub") * lax.axis_size("pair")
    pages = prepare(counts, probs.T, defocus[None], classes.T, poses.T, spectra)
    other_pages = shift(pages, "pair", 1)
    place = jnp.stack([lax.axis_index("pair"), lax.axis_index("parts")])
    col_rows = jnp.swapaxes(col_kernel, 1, 2)
    parts = insert_particles(place, offsets, row_kernel, col_rows, pages, other_pages, n_class)
    planes = lax.all_gather(sum_at_owner(parts, "parts"), ("sub", "pair"), axis=0, tiled=False)
    mix_rows, mix_cols, last_rows, last_cols = tables(group)
    mine = lax.dynamic_index_in_dim(jnp.asarray(last_cols), lax.axis_index(("sub", "pair")), 1, keepdims=False)
    copies = refine_class(
        planes, jnp.asarray(mix_rows), jnp.asarray(mix_cols), jnp.asarray(last_rows), mine, n_class // NEAR
    )
    return from_all(copies, "parts", place)


def solution(mesh):
    shards = ("groups", "parts", "pair")
    placed = (
        P(shards, None, None),
        P(shards),
        P(shards, None),
        P(shards, None),
        P(shards, None),
        P(shards),
        P(),
        P(None, "sub", None),
        P(),
    )
    return jax.shard_map(
        per_device,
        mesh=mesh,
        in_specs=placed,
        out_specs=P("groups", ("sub", "pair"), None),
        check_vma=False,
    )
```

```python
import functools
import math

import jax
import jax.numpy as jnp
import numpy as np
from jax import lax
from jax.experimental import pallas as pl
from jax.experimental.pallas import tpu as pltpu
from jax.sharding import PartitionSpec as P

GRID = 512
BOX = 256
IROWS = 128
ICOLS = 64
LROWS = 256
LCOLS = 128
BAND = 64
K_TOP = 4
ITERS = 4
LANES = 128
UNROLL = 4
ALL_VMEM = 67043328
WEIGHTS, DEFOCUS, CLASSES, POSES, COUNT, SMALL = 0, K_TOP, K_TOP + 1, 2 * K_TOP + 1, 3 * K_TOP + 1, 16
NEAR = 4

blob_width = 1.5
avg_scale = 8.0
floor_value = 1.0

F32 = jnp.float32
BF16 = jnp.bfloat16
NT = (((1,), (1,)), ((), ()))
NN = (((1,), (0,)), ((), ()))


def sine_terms():
    r = np.cos(np.linspace(0.0, np.pi, 4001)) * 0.5
    r = r[np.abs(r) > 1e-3]
    z = r * r
    powers = np.stack([z**k for k in range(6)], axis=1)
    terms, *_ = np.linalg.lstsq(powers, np.sin(np.pi * r) / r, rcond=None)
    return [float(t) for t in terms]


SINE = sine_terms()


def start_all(pairs, sems):
    copies = [pltpu.make_async_copy(source, target, sems.at[i]) for i, (source, target) in enumerate(pairs)]
    for copy in copies:
        copy.start()
    return copies


def prepare_kernel(
    counts_in, probs_in, defocus_in, classes_in, poses_in, spec_in,
    pages_ref, counts_ref, probs_ref, defocus_ref, classes_ref, poses_ref, small_ref, sems,
):
    n_slots = spec_in.shape[0]
    copies = start_all(
        [
            (spec_in, pages_ref.at[pl.ds(0, n_slots)]),
            (counts_in, counts_ref),
            (probs_in, probs_ref),
            (defocus_in, defocus_ref),
            (classes_in, classes_ref),
            (poses_in, poses_ref),
        ],
        sems,
    )
    small_ref[...] = jnp.zeros_like(small_ref)
    pages_ref[n_slots] = jnp.zeros(pages_ref.shape[1:], BF16)
    for copy in copies[1:]:
        copy.wait()
    used = lax.broadcasted_iota(jnp.int32, (K_TOP, n_slots), 1) < counts_ref[0]
    small_ref[WEIGHTS : WEIGHTS + K_TOP, :n_slots] = jnp.where(used, probs_ref[...].astype(F32), 0.0)
    small_ref[DEFOCUS : DEFOCUS + 1, :n_slots] = defocus_ref[...].astype(F32)
    small_ref[CLASSES : CLASSES + K_TOP, :n_slots] = classes_ref[...].astype(F32)
    small_ref[POSES : POSES + K_TOP, :n_slots] = poses_ref[...].astype(F32)
    small_ref[COUNT : COUNT + 1, :] = jnp.full((1, LANES), counts_ref[0], jnp.int32).astype(F32)
    pages_ref[n_slots, :SMALL] = small_ref[...].astype(BF16)
    copies[0].wait()


def prepare(counts, probs, defocus, classes, poses, spectra):
    n_slots = spectra.shape[0]
    return pl.pallas_call(
        prepare_kernel,
        out_shape=jax.ShapeDtypeStruct((n_slots + 1, IROWS, LANES), BF16),
        in_specs=[pl.BlockSpec(memory_space=pl.ANY)] * 6,
        out_specs=pl.BlockSpec(memory_space=pltpu.VMEM),
        scratch_shapes=[
            pltpu.SMEM(counts.shape, jnp.int32),
            pltpu.VMEM(probs.shape, BF16),
            pltpu.VMEM(defocus.shape, BF16),
            pltpu.VMEM(classes.shape, jnp.int32),
            pltpu.VMEM(poses.shape, jnp.int32),
            pltpu.VMEM((SMALL, LANES), F32),
            pltpu.SemaphoreType.DMA((6,)),
        ],
        cost_estimate=pl.CostEstimate(flops=10**6, bytes_accessed=2 * 10**6, transcendentals=0),
        compiler_params=pltpu.CompilerParams(vmem_limit_bytes=ALL_VMEM),
        name="prepare",
    )(counts, probs, defocus, classes, poses, spectra)


def particle_kernel(
    place_ref, offsets_in, rk_in, ck_in, own_in, other_in,
    out0_ref, out1_ref, out2_ref, out2b_ref, out3_ref,
    offsets_ref, rows_ref, cols_ref, pages_ref, placed_ref, total_ref, radius_ref, page_ref, small_ref, scalars_ref, sems,
):
    n_slots = pages_ref.shape[1]
    n_class = total_ref.shape[0]
    n_pose, half = placed_ref.shape[0], placed_ref.shape[1]
    first_row = pl.multiple_of(place_ref[0] * half, half)
    here = place_ref[1]
    copies = start_all(
        [
            (own_in.at[n_slots, pl.ds(0, SMALL)], page_ref.at[0]),
            (other_in.at[n_slots, pl.ds(0, SMALL)], page_ref.at[1]),
            (offsets_in, offsets_ref),
            (rk_in.at[:, pl.ds(first_row, half), :], rows_ref),
            (own_in.at[pl.ds(0, n_slots)], pages_ref.at[0]),
            (ck_in, cols_ref),
            (other_in.at[pl.ds(0, n_slots)], pages_ref.at[1]),
        ],
        sems,
    )
    lane = lax.broadcasted_iota(jnp.int32, (1, LANES), 1)
    low = lane < ICOLS
    packed = (IROWS // 2, LANES)
    row_freq = lax.broadcasted_iota(jnp.int32, packed, 0) - jnp.where(low, IROWS // 2, 0)
    row_freq = row_freq.astype(F32)
    col_freq = (lax.broadcasted_iota(jnp.int32, packed, 1) & (ICOLS - 1)).astype(F32)
    radius_ref[...] = (row_freq * row_freq + col_freq * col_freq) * (10.0 / (ICOLS * ICOLS))
    total_ref[...] = jnp.zeros_like(total_ref)
    copies[0].wait()
    copies[1].wait()
    small_ref[...] = page_ref[...].astype(F32)
    scalars = pltpu.make_async_copy(small_ref, scalars_ref, sems.at[7])
    scalars.start()
    copies[2].wait()
    copies[3].wait()
    for b in range(n_pose):
        band = rows_ref[b].astype(F32)
        band = jnp.concatenate([band, jnp.zeros((half, LANES - BAND), F32)], axis=1)
        placed_ref[b] = pltpu.roll(band, offsets_ref[b], 1).astype(BF16)
    scalars.wait()
    for copy in copies[4:]:
        copy.wait()

    def pick(shard, row, n):
        return scalars_ref[shard, row, n].astype(jnp.int32)

    blocks = [(pick(shard, COUNT, 0) + UNROLL - 1) // UNROLL for shard in range(2)]

    def step(block, carry):
        shard = (block >= blocks[0]).astype(jnp.int32)
        first = (block - shard * blocks[0]) * UNROLL
        sums = []
        for u in range(UNROLL):
            n = first + u
            turns = radius_ref[...] * scalars_ref[shard, DEFOCUS, n]
            turns = turns - jnp.floor(turns + 0.5)
            t = 2.0 * turns + 0.1 / math.pi
            k = jnp.floor(t + 0.5)
            r = t - k
            z = r * r
            s = SINE[-1]
            for term in SINE[-2::-1]:
                s = s * z + term
            ctf = s * r * (1.0 - 2.0 * k * k)
            turned = pltpu.roll(ctf, ICOLS, 1)
            ctf = jnp.concatenate([jnp.where(low, ctf, turned), jnp.where(low, turned, ctf)], axis=0)
            data = (ctf * pages_ref[shard, n].astype(F32)).astype(BF16)
            power = jnp.where(low, ctf * ctf, 0.0).astype(BF16)
            planes = jnp.concatenate([data, power], axis=1)
            poses = [pick(shard, POSES + j, n) for j in range(K_TOP)]
            rows = jnp.concatenate([placed_ref[b] for b in poses], axis=0)
            mixed = lax.dot_general(rows, planes, NN, preferred_element_type=F32)
            for j in range(K_TOP):
                m = mixed[j * half : (j + 1) * half] * scalars_ref[shard, WEIGHTS + j, n]
                pair = m[:, :LANES]
                stacked = jnp.concatenate(
                    [jnp.where(low, pair, 0.0), jnp.where(low, 0.0, pair), m[:, LANES:]], axis=0
                ).astype(BF16)
                cols = cols_ref[poses[j]]
                cols = jnp.concatenate([cols, cols], axis=0)
                spread = lax.dot_general(stacked, cols, NN, preferred_element_type=F32)
                c = pick(shard, CLASSES + j, n)
                d = (c + n_class - here) % NEAR
                sums.append((d * (n_class // NEAR) + c // NEAR, spread))
        for c, spread in sums:
            total_ref[c] += spread
        return carry

    lax.fori_loop(0, blocks[0] + blocks[1], step, 0)
    first = 0
    for out_ref in (out0_ref, out1_ref, out2_ref, out2b_ref, out3_ref):
        out_ref[...] = total_ref[first : first + out_ref.shape[0]].astype(out_ref.dtype)
        first += out_ref.shape[0]


def insert_particles(place, offsets, row_kernel, col_kernel, pages, other_pages, n_class):
    n_pose, rows, _ = row_kernel.shape
    half = rows // 2
    out = (n_class, 3 * half, LCOLS)
    each = n_class // NEAR
    sizes = (each, each, each // 2, each - each // 2, each)
    work = 2 * (pages.shape[0] - 1) * K_TOP * half * 2
    return pl.pallas_call(
        particle_kernel,
        out_shape=[jax.ShapeDtypeStruct((size, *out[1:]), BF16) for size in sizes],
        in_specs=[pl.BlockSpec(memory_space=pltpu.SMEM)] + [pl.BlockSpec(memory_space=pl.ANY)] * 5,
        out_specs=[pl.BlockSpec(memory_space=pltpu.VMEM)] * len(sizes),
        scratch_shapes=[
            pltpu.SMEM(offsets.shape, jnp.int32),
            pltpu.VMEM((n_pose, half, BAND), BF16),
            pltpu.VMEM(col_kernel.shape, BF16),
            pltpu.VMEM((2, pages.shape[0] - 1, *pages.shape[1:]), BF16),
            pltpu.VMEM((n_pose, half, LANES), BF16),
            pltpu.VMEM(out, F32),
            pltpu.VMEM((IROWS // 2, LANES), F32),
            pltpu.VMEM((2, SMALL, LANES), BF16),
            pltpu.VMEM((2, SMALL, LANES), F32),
            pltpu.SMEM((2, SMALL, LANES), F32),
            pltpu.SemaphoreType.DMA((8,)),
        ],
        cost_estimate=pl.CostEstimate(
            flops=work * (IROWS * 2 * LANES + 3 * LANES * LCOLS) * 8,
            bytes_accessed=2 * 2 * math.prod(out),
            transcendentals=0,
        ),
        compiler_params=pltpu.CompilerParams(vmem_limit_bytes=ALL_VMEM),
        name="insert_particles",
    )(place, offsets, row_kernel, col_kernel, pages, other_pages)


def split_bf16(x):
    hi = x.astype(BF16)
    return hi, (x - hi.astype(F32)).astype(BF16)


def dot3(a, b, dims):
    (ah, al), (bh, bl) = a, b
    dot = functools.partial(lax.dot_general, dimension_numbers=dims, preferred_element_type=F32)
    return dot(ah, bh) + (dot(ah, bl) + dot(al, bh))


@functools.cache
def tables(groups):
    grid = np.arange(GRID)
    distance = np.minimum(grid, GRID - grid).astype(np.float64)
    blob = np.exp(-2.0 * np.pi**2 * blob_width**2 * distance**2 / GRID**2)
    angle = 2.0 * np.pi / GRID
    kernel = np.cos(angle * (grid[:, None] * grid[None, :] % GRID)) @ blob / GRID
    rows = np.arange(LROWS) - LROWS // 2
    cols = np.arange(LCOLS)
    factor = np.where(cols == 0, 1.0, 2.0)
    mix_rows = np.concatenate(
        [kernel[(rows[:, None] - rows[None, :]) % GRID], kernel[(rows[:, None] + rows[None, :]) % GRID]], axis=1
    )
    half = 0.5 * factor[:, None]
    mix_cols = np.concatenate(
        [half * kernel[(cols[:, None] - cols[None, :]) % GRID], half * kernel[(cols[:, None] + cols[None, :]) % GRID]],
        axis=1,
    )
    crop = np.arange(BOX) - BOX // 2
    correction = np.sinc(crop / GRID) ** 2
    row_angle = angle * (rows[:, None] * crop[None, :] % GRID)
    last_rows = np.concatenate([np.cos(row_angle), -np.sin(row_angle)], axis=0)
    last_rows = last_rows * (avg_scale / GRID) / correction[None, :]
    col_angle = angle * (crop[:, None] * cols[None, :] % GRID)
    last_cols = np.stack([np.cos(col_angle), np.sin(col_angle)], axis=0)
    last_cols = last_cols * factor[None, None, :] / correction[None, :, None]
    last_cols = last_cols.reshape(2, groups, BOX // groups, LCOLS).transpose(1, 0, 2, 3)
    last_cols = last_cols.reshape(groups, 2 * (BOX // groups), LCOLS)

    def two(x):
        x = x.astype(np.float32)
        hi = x.astype(jnp.bfloat16)
        lo = (x - hi.astype(np.float32)).astype(jnp.bfloat16)
        return np.stack([hi, lo])

    return two(mix_rows), two(mix_cols), two(last_rows), two(last_cols)


def refine_kernel(planes_ref, mix_rows_ref, mix_cols_ref, last_rows_ref, last_cols_ref, out_ref):
    blocks, third = planes_ref.shape[0], planes_ref.shape[1] // 3

    def plane(p):
        return jnp.concatenate([planes_ref[g, p * third : (p + 1) * third] for g in range(blocks)], axis=0).astype(F32)

    weight = plane(2)
    mix_rows = (mix_rows_ref[0], mix_rows_ref[1])
    mix_cols = (mix_cols_ref[0], mix_cols_ref[1])
    scale = jnp.ones_like(weight)
    for _ in range(ITERS):
        half = dot3(split_bf16(weight * scale), mix_cols, NN)
        half = jnp.concatenate([half[:, :LCOLS], half[:, LCOLS:]], axis=0)
        conv = dot3(mix_rows, split_bf16(half), NN)
        scale = scale / jnp.maximum(jnp.abs(conv), floor_value)
    last_cols = (last_cols_ref[0], last_cols_ref[1])
    real = dot3(last_cols, split_bf16(plane(0) * scale), NT)
    imag = dot3(last_cols, split_bf16(plane(1) * scale), NT)
    n = real.shape[0] // 2
    both = jnp.concatenate([real[:n] - imag[n:], real[n:] + imag[:n]], axis=1)
    out = dot3(split_bf16(both), (last_rows_ref[0], last_rows_ref[1]), NN)
    for i in range(out_ref.shape[0]):
        out_ref[i] = out.astype(out_ref.dtype)


def refine_class(planes, mix_rows, mix_cols, last_rows, last_cols, n_copies):
    vmem = pl.BlockSpec(memory_space=pltpu.VMEM)
    return pl.pallas_call(
        refine_kernel,
        out_shape=jax.ShapeDtypeStruct((n_copies, last_cols.shape[1] // 2, BOX), BF16),
        in_specs=[vmem] * 5,
        out_specs=vmem,
        cost_estimate=pl.CostEstimate(flops=2 * 10**9, bytes_accessed=3 * 10**6, transcendentals=0),
        compiler_params=pltpu.CompilerParams(vmem_limit_bytes=32 * 2**20),
        name="refine_class",
    )(planes, mix_rows, mix_cols, last_rows, last_cols)


def shift(value, axis, by):
    n = lax.axis_size(axis)
    return lax.ppermute(value, axis, [(i, (i + by) % n) for i in range(n)])


def strided(n, stride):
    return [list(range(first, n, stride)) for first in range(stride)]


def added(parts):
    total = parts[0].astype(F32)
    for i in range(1, len(parts)):
        total = total + parts[i].astype(F32)
    return total


def collect_kernel(a_ref, b_ref, low_ref, high_ref, d_ref, out_ref):
    n_low = low_ref.shape[0]
    out_ref[:n_low] = added([a_ref[:n_low], b_ref[:n_low], low_ref[...], d_ref[:n_low]]).astype(out_ref.dtype)
    out_ref[n_low:] = added([a_ref[n_low:], b_ref[n_low:], high_ref[...], d_ref[n_low:]]).astype(out_ref.dtype)


def collect(*parts):
    vmem = pl.BlockSpec(memory_space=pltpu.VMEM)
    return pl.pallas_call(
        collect_kernel,
        out_shape=jax.ShapeDtypeStruct(parts[0].shape, BF16),
        in_specs=[vmem] * len(parts),
        out_specs=vmem,
        cost_estimate=pl.CostEstimate(flops=10**6, bytes_accessed=10**6, transcendentals=0),
        compiler_params=pltpu.CompilerParams(vmem_limit_bytes=8 * 2**20),
        name="collect",
    )(*parts)


def sum_at_owner(parts, axis):
    here = collect(
        parts[0],
        shift(parts[1], axis, 1),
        shift(parts[2], axis, 2),
        shift(parts[3], axis, -2),
        shift(parts[4], axis, -1),
    )
    return added(lax.all_to_all(here, axis, 0, 0, axis_index_groups=strided(lax.axis_size(axis), NEAR)))


def place_kernel(place_ref, own_ref, *refs):
    out_ref = refs[-1]
    n_class = out_ref.shape[0]
    for ref, d in zip((own_ref, *refs[:-1]), (0, 1, 2, -1)):
        first = (place_ref[1] + d + n_class) % NEAR
        for i in range(own_ref.shape[0]):
            out_ref[NEAR * i + first] = ref[i].astype(F32)


def from_all(copies, axis, place):
    n = lax.axis_size(axis)
    own = lax.all_to_all(copies, axis, 0, 0, axis_index_groups=strided(n, NEAR))
    near = [shift(own, axis, -1), shift(own, axis, -2), shift(own, axis, 1)]
    vmem = pl.BlockSpec(memory_space=pltpu.VMEM)
    return pl.pallas_call(
        place_kernel,
        out_shape=jax.ShapeDtypeStruct((n, *copies.shape[1:]), F32),
        in_specs=[pl.BlockSpec(memory_space=pltpu.SMEM)] + [vmem] * NEAR,
        out_specs=vmem,
        cost_estimate=pl.CostEstimate(flops=10**6, bytes_accessed=2 * 10**6, transcendentals=0),
        compiler_params=pltpu.CompilerParams(vmem_limit_bytes=16 * 2**20),
        name="place_averages",
    )(place, own, *near)


def per_device(spectra, defocus, classes, poses, probs, counts, offsets, row_kernel, col_kernel):
    n_class = lax.axis_size("parts")
    group = lax.axis_size("sub") * lax.axis_size("pair")
    pages = prepare(counts, probs.T, defocus[None], classes.T, poses.T, spectra)
    other_pages = shift(pages, "pair", 1)
    place = jnp.stack([lax.axis_index("pair"), lax.axis_index("parts")])
    col_rows = jnp.swapaxes(col_kernel, 1, 2)
    parts = insert_particles(place, offsets, row_kernel, col_rows, pages, other_pages, n_class)
    planes = lax.all_gather(sum_at_owner(parts, "parts"), ("sub", "pair"), axis=0, tiled=False)
    mix_rows, mix_cols, last_rows, last_cols = tables(group)
    mine = lax.dynamic_index_in_dim(jnp.asarray(last_cols), lax.axis_index(("sub", "pair")), 1, keepdims=False)
    copies = refine_class(
        planes, jnp.asarray(mix_rows), jnp.asarray(mix_cols), jnp.asarray(last_rows), mine, n_class // NEAR
    )
    return from_all(copies, "parts", place)


def solution(mesh):
    shards = ("groups", "parts", "pair")
    placed = (
        P(shards, None, None),
        P(shards),
        P(shards, None),
        P(shards, None),
        P(shards, None),
        P(shards),
        P(),
        P(None, "sub", None),
        P(),
    )
    return jax.shard_map(
        per_device,
        mesh=mesh,
        in_specs=placed,
        out_specs=P("groups", ("sub", "pair"), None),
        check_vma=False,
    )
```

```python
import functools
import math

import jax
import jax.numpy as jnp
import numpy as np
from jax import lax
from jax.experimental import pallas as pl
from jax.experimental.pallas import tpu as pltpu
from jax.sharding import PartitionSpec as P

GRID = 512
BOX = 256
IROWS = 128
ICOLS = 64
LROWS = 256
LCOLS = 128
BAND = 64
K_TOP = 4
ITERS = 4
LANES = 128
UNROLL = 4
ALL_VMEM = 67043328
WEIGHTS, DEFOCUS, CLASSES, POSES, COUNT, SMALL = 0, K_TOP, K_TOP + 1, 2 * K_TOP + 1, 3 * K_TOP + 1, 16
NEAR = 4

blob_width = 1.5
avg_scale = 8.0
floor_value = 1.0

F32 = jnp.float32
BF16 = jnp.bfloat16
NT = (((1,), (1,)), ((), ()))
NN = (((1,), (0,)), ((), ()))


def sine_terms():
    r = np.cos(np.linspace(0.0, np.pi, 4001)) * 0.5
    r = r[np.abs(r) > 1e-3]
    z = r * r
    powers = np.stack([z**k for k in range(6)], axis=1)
    terms, *_ = np.linalg.lstsq(powers, np.sin(np.pi * r) / r, rcond=None)
    return [float(t) for t in terms]


SINE = sine_terms()


def start_all(pairs, sems):
    copies = [pltpu.make_async_copy(source, target, sems.at[i]) for i, (source, target) in enumerate(pairs)]
    for copy in copies:
        copy.start()
    return copies


def prepare_kernel(
    counts_in, probs_in, defocus_in, classes_in, poses_in, spec_in,
    pages_ref, counts_ref, probs_ref, defocus_ref, classes_ref, poses_ref, small_ref, sems,
):
    n_slots = spec_in.shape[0]
    copies = start_all(
        [
            (spec_in, pages_ref.at[pl.ds(0, n_slots)]),
            (counts_in, counts_ref),
            (probs_in, probs_ref),
            (defocus_in, defocus_ref),
            (classes_in, classes_ref),
            (poses_in, poses_ref),
        ],
        sems,
    )
    small_ref[...] = jnp.zeros_like(small_ref)
    pages_ref[n_slots] = jnp.zeros(pages_ref.shape[1:], BF16)
    for copy in copies[1:]:
        copy.wait()
    used = lax.broadcasted_iota(jnp.int32, (K_TOP, n_slots), 1) < counts_ref[0]
    small_ref[WEIGHTS : WEIGHTS + K_TOP, :n_slots] = jnp.where(used, probs_ref[...].astype(F32), 0.0)
    small_ref[DEFOCUS : DEFOCUS + 1, :n_slots] = defocus_ref[...].astype(F32)
    small_ref[CLASSES : CLASSES + K_TOP, :n_slots] = classes_ref[...].astype(F32)
    small_ref[POSES : POSES + K_TOP, :n_slots] = poses_ref[...].astype(F32)
    small_ref[COUNT : COUNT + 1, :] = jnp.full((1, LANES), counts_ref[0], jnp.int32).astype(F32)
    pages_ref[n_slots, :SMALL] = small_ref[...].astype(BF16)
    copies[0].wait()


def prepare(counts, probs, defocus, classes, poses, spectra):
    n_slots = spectra.shape[0]
    return pl.pallas_call(
        prepare_kernel,
        out_shape=jax.ShapeDtypeStruct((n_slots + 1, IROWS, LANES), BF16),
        in_specs=[pl.BlockSpec(memory_space=pl.ANY)] * 6,
        out_specs=pl.BlockSpec(memory_space=pltpu.VMEM),
        scratch_shapes=[
            pltpu.SMEM(counts.shape, jnp.int32),
            pltpu.VMEM(probs.shape, BF16),
            pltpu.VMEM(defocus.shape, BF16),
            pltpu.VMEM(classes.shape, jnp.int32),
            pltpu.VMEM(poses.shape, jnp.int32),
            pltpu.VMEM((SMALL, LANES), F32),
            pltpu.SemaphoreType.DMA((6,)),
        ],
        cost_estimate=pl.CostEstimate(flops=10**6, bytes_accessed=2 * 10**6, transcendentals=0),
        compiler_params=pltpu.CompilerParams(vmem_limit_bytes=ALL_VMEM),
        name="prepare",
    )(counts, probs, defocus, classes, poses, spectra)


def particle_kernel(
    place_ref, offsets_in, rk_in, ck_in, own_in, other_in,
    out0_ref, out1_ref, out2_ref, out3_ref,
    offsets_ref, rows_ref, cols_ref, pages_ref, placed_ref, total_ref, radius_ref, page_ref, small_ref, scalars_ref, sems,
):
    n_slots = pages_ref.shape[1]
    n_class = total_ref.shape[0]
    n_pose, half = placed_ref.shape[0], placed_ref.shape[1]
    first_row = pl.multiple_of(place_ref[0] * half, half)
    here = place_ref[1]
    copies = start_all(
        [
            (own_in.at[n_slots, pl.ds(0, SMALL)], page_ref.at[0]),
            (other_in.at[n_slots, pl.ds(0, SMALL)], page_ref.at[1]),
            (offsets_in, offsets_ref),
            (rk_in.at[:, pl.ds(first_row, half), :], rows_ref),
            (own_in.at[pl.ds(0, n_slots)], pages_ref.at[0]),
            (ck_in, cols_ref),
            (other_in.at[pl.ds(0, n_slots)], pages_ref.at[1]),
        ],
        sems,
    )
    lane = lax.broadcasted_iota(jnp.int32, (1, LANES), 1)
    low = lane < ICOLS
    packed = (IROWS // 2, LANES)
    row_freq = lax.broadcasted_iota(jnp.int32, packed, 0) - jnp.where(low, IROWS // 2, 0)
    row_freq = row_freq.astype(F32)
    col_freq = (lax.broadcasted_iota(jnp.int32, packed, 1) & (ICOLS - 1)).astype(F32)
    radius_ref[...] = (row_freq * row_freq + col_freq * col_freq) * (10.0 / (ICOLS * ICOLS))
    total_ref[...] = jnp.zeros_like(total_ref)
    copies[0].wait()
    copies[1].wait()
    small_ref[...] = page_ref[...].astype(F32)
    scalars = pltpu.make_async_copy(small_ref, scalars_ref, sems.at[7])
    scalars.start()
    copies[2].wait()
    copies[3].wait()
    for b in range(n_pose):
        band = rows_ref[b].astype(F32)
        band = jnp.concatenate([band, jnp.zeros((half, LANES - BAND), F32)], axis=1)
        placed_ref[b] = pltpu.roll(band, offsets_ref[b], 1).astype(BF16)
    scalars.wait()
    for copy in copies[4:]:
        copy.wait()

    def pick(shard, row, n):
        return scalars_ref[shard, row, n].astype(jnp.int32)

    blocks = [(pick(shard, COUNT, 0) + UNROLL - 1) // UNROLL for shard in range(2)]

    def step(block, carry):
        shard = (block >= blocks[0]).astype(jnp.int32)
        first = (block - shard * blocks[0]) * UNROLL
        sums = []
        for u in range(UNROLL):
            n = first + u
            turns = radius_ref[...] * scalars_ref[shard, DEFOCUS, n]
            turns = turns - jnp.floor(turns + 0.5)
            t = 2.0 * turns + 0.1 / math.pi
            k = jnp.floor(t + 0.5)
            r = t - k
            z = r * r
            s = SINE[-1]
            for term in SINE[-2::-1]:
                s = s * z + term
            ctf = s * r * (1.0 - 2.0 * k * k)
            turned = pltpu.roll(ctf, ICOLS, 1)
            ctf = jnp.concatenate([jnp.where(low, ctf, turned), jnp.where(low, turned, ctf)], axis=0)
            data = (ctf * pages_ref[shard, n].astype(F32)).astype(BF16)
            power = jnp.where(low, ctf * ctf, 0.0).astype(BF16)
            planes = jnp.concatenate([data, power], axis=1)
            poses = [pick(shard, POSES + j, n) for j in range(K_TOP)]
            rows = jnp.concatenate([placed_ref[b] for b in poses], axis=0)
            mixed = lax.dot_general(rows, planes, NN, preferred_element_type=F32)
            for j in range(K_TOP):
                m = mixed[j * half : (j + 1) * half] * scalars_ref[shard, WEIGHTS + j, n]
                pair = m[:, :LANES]
                stacked = jnp.concatenate(
                    [jnp.where(low, pair, 0.0), jnp.where(low, 0.0, pair), m[:, LANES:]], axis=0
                ).astype(BF16)
                cols = cols_ref[poses[j]]
                cols = jnp.concatenate([cols, cols], axis=0)
                spread = lax.dot_general(stacked, cols, NN, preferred_element_type=F32)
                c = pick(shard, CLASSES + j, n)
                d = (c + n_class - here) % NEAR
                sums.append((d * (n_class // NEAR) + c // NEAR, spread))
        for c, spread in sums:
            total_ref[c] += spread
        return carry

    lax.fori_loop(0, blocks[0] + blocks[1], step, 0)
    for d, out_ref in enumerate((out0_ref, out1_ref, out2_ref, out3_ref)):
        out_ref[...] = total_ref[pl.ds(d * (n_class // NEAR), n_class // NEAR)].astype(out_ref.dtype)


def insert_particles(place, offsets, row_kernel, col_kernel, pages, other_pages, n_class):
    n_pose, rows, _ = row_kernel.shape
    half = rows // 2
    out = (n_class, 3 * half, LCOLS)
    work = 2 * (pages.shape[0] - 1) * K_TOP * half * 2
    return pl.pallas_call(
        particle_kernel,
        out_shape=[jax.ShapeDtypeStruct((n_class // NEAR, *out[1:]), BF16)] * NEAR,
        in_specs=[pl.BlockSpec(memory_space=pltpu.SMEM)] + [pl.BlockSpec(memory_space=pl.ANY)] * 5,
        out_specs=[pl.BlockSpec(memory_space=pltpu.VMEM)] * NEAR,
        scratch_shapes=[
            pltpu.SMEM(offsets.shape, jnp.int32),
            pltpu.VMEM((n_pose, half, BAND), BF16),
            pltpu.VMEM(col_kernel.shape, BF16),
            pltpu.VMEM((2, pages.shape[0] - 1, *pages.shape[1:]), BF16),
            pltpu.VMEM((n_pose, half, LANES), BF16),
            pltpu.VMEM(out, F32),
            pltpu.VMEM((IROWS // 2, LANES), F32),
            pltpu.VMEM((2, SMALL, LANES), BF16),
            pltpu.VMEM((2, SMALL, LANES), F32),
            pltpu.SMEM((2, SMALL, LANES), F32),
            pltpu.SemaphoreType.DMA((8,)),
        ],
        cost_estimate=pl.CostEstimate(
            flops=work * (IROWS * 2 * LANES + 3 * LANES * LCOLS) * 8,
            bytes_accessed=2 * 2 * math.prod(out),
            transcendentals=0,
        ),
        compiler_params=pltpu.CompilerParams(vmem_limit_bytes=ALL_VMEM),
        name="insert_particles",
    )(place, offsets, row_kernel, col_kernel, pages, other_pages)


def split_bf16(x):
    hi = x.astype(BF16)
    return hi, (x - hi.astype(F32)).astype(BF16)


def dot3(a, b, dims):
    (ah, al), (bh, bl) = a, b
    dot = functools.partial(lax.dot_general, dimension_numbers=dims, preferred_element_type=F32)
    return dot(ah, bh) + (dot(ah, bl) + dot(al, bh))


@functools.cache
def tables(groups):
    grid = np.arange(GRID)
    distance = np.minimum(grid, GRID - grid).astype(np.float64)
    blob = np.exp(-2.0 * np.pi**2 * blob_width**2 * distance**2 / GRID**2)
    angle = 2.0 * np.pi / GRID
    kernel = np.cos(angle * (grid[:, None] * grid[None, :] % GRID)) @ blob / GRID
    rows = np.arange(LROWS) - LROWS // 2
    cols = np.arange(LCOLS)
    factor = np.where(cols == 0, 1.0, 2.0)
    mix_rows = np.concatenate(
        [kernel[(rows[:, None] - rows[None, :]) % GRID], kernel[(rows[:, None] + rows[None, :]) % GRID]], axis=1
    )
    half = 0.5 * factor[:, None]
    mix_cols = np.concatenate(
        [half * kernel[(cols[:, None] - cols[None, :]) % GRID], half * kernel[(cols[:, None] + cols[None, :]) % GRID]],
        axis=1,
    )
    crop = np.arange(BOX) - BOX // 2
    correction = np.sinc(crop / GRID) ** 2
    row_angle = angle * (rows[:, None] * crop[None, :] % GRID)
    last_rows = np.concatenate([np.cos(row_angle), -np.sin(row_angle)], axis=0)
    last_rows = last_rows * (avg_scale / GRID) / correction[None, :]
    col_angle = angle * (crop[:, None] * cols[None, :] % GRID)
    last_cols = np.stack([np.cos(col_angle), np.sin(col_angle)], axis=0)
    last_cols = last_cols * factor[None, None, :] / correction[None, :, None]
    last_cols = last_cols.reshape(2, groups, BOX // groups, LCOLS).transpose(1, 0, 2, 3)
    last_cols = last_cols.reshape(groups, 2 * (BOX // groups), LCOLS)

    def two(x):
        x = x.astype(np.float32)
        hi = x.astype(jnp.bfloat16)
        lo = (x - hi.astype(np.float32)).astype(jnp.bfloat16)
        return np.stack([hi, lo])

    return two(mix_rows), two(mix_cols), two(last_rows), two(last_cols)


def refine_kernel(planes_ref, mix_rows_ref, mix_cols_ref, last_rows_ref, last_cols_ref, out_ref):
    blocks, third = planes_ref.shape[0], planes_ref.shape[1] // 3

    def plane(p):
        return jnp.concatenate([planes_ref[g, p * third : (p + 1) * third] for g in range(blocks)], axis=0).astype(F32)

    weight = plane(2)
    mix_rows = (mix_rows_ref[0], mix_rows_ref[1])
    mix_cols = (mix_cols_ref[0], mix_cols_ref[1])
    scale = jnp.ones_like(weight)
    for _ in range(ITERS):
        half = dot3(split_bf16(weight * scale), mix_cols, NN)
        half = jnp.concatenate([half[:, :LCOLS], half[:, LCOLS:]], axis=0)
        conv = dot3(mix_rows, split_bf16(half), NN)
        scale = scale / jnp.maximum(jnp.abs(conv), floor_value)
    last_cols = (last_cols_ref[0], last_cols_ref[1])
    real = dot3(last_cols, split_bf16(plane(0) * scale), NT)
    imag = dot3(last_cols, split_bf16(plane(1) * scale), NT)
    n = real.shape[0] // 2
    both = jnp.concatenate([real[:n] - imag[n:], real[n:] + imag[:n]], axis=1)
    out = dot3(split_bf16(both), (last_rows_ref[0], last_rows_ref[1]), NN)
    for i in range(out_ref.shape[0]):
        out_ref[i] = out.astype(out_ref.dtype)


def refine_class(planes, mix_rows, mix_cols, last_rows, last_cols, n_copies):
    vmem = pl.BlockSpec(memory_space=pltpu.VMEM)
    return pl.pallas_call(
        refine_kernel,
        out_shape=jax.ShapeDtypeStruct((n_copies, last_cols.shape[1] // 2, BOX), BF16),
        in_specs=[vmem] * 5,
        out_specs=vmem,
        cost_estimate=pl.CostEstimate(flops=2 * 10**9, bytes_accessed=3 * 10**6, transcendentals=0),
        compiler_params=pltpu.CompilerParams(vmem_limit_bytes=32 * 2**20),
        name="refine_class",
    )(planes, mix_rows, mix_cols, last_rows, last_cols)


def shift(value, axis, by):
    n = lax.axis_size(axis)
    return lax.ppermute(value, axis, [(i, (i + by) % n) for i in range(n)])


def strided(n, stride):
    return [list(range(first, n, stride)) for first in range(stride)]


def added(parts):
    total = parts[0].astype(F32)
    for i in range(1, len(parts)):
        total = total + parts[i].astype(F32)
    return total


def collect_kernel(a_ref, b_ref, c_ref, d_ref, out_ref):
    out_ref[...] = added([a_ref[...], b_ref[...], c_ref[...], d_ref[...]]).astype(out_ref.dtype)


def collect(parts):
    vmem = pl.BlockSpec(memory_space=pltpu.VMEM)
    return pl.pallas_call(
        collect_kernel,
        out_shape=jax.ShapeDtypeStruct(parts[0].shape, BF16),
        in_specs=[vmem] * NEAR,
        out_specs=vmem,
        cost_estimate=pl.CostEstimate(flops=10**6, bytes_accessed=10**6, transcendentals=0),
        compiler_params=pltpu.CompilerParams(vmem_limit_bytes=8 * 2**20),
        name="collect",
    )(*parts)


def sum_at_owner(parts, axis):
    here = collect([parts[0], shift(parts[1], axis, 1), shift(parts[2], axis, 2), shift(parts[3], axis, -1)])
    return added(lax.all_to_all(here, axis, 0, 0, axis_index_groups=strided(lax.axis_size(axis), NEAR)))


def neighbours(n, size):
    return [[first + i for i in range(size)] for first in range(0, n, size)]


def from_all(copies, axis):
    n = lax.axis_size(axis)
    far = lax.all_to_all(copies, axis, 0, 0, axis_index_groups=strided(n, NEAR))
    far = jnp.broadcast_to(far, (NEAR, *far.shape))
    every = lax.all_to_all(far, axis, 0, 0, axis_index_groups=neighbours(n, NEAR))
    return jnp.swapaxes(every, 0, 1).reshape(n, *copies.shape[1:])


def per_device(spectra, defocus, classes, poses, probs, counts, offsets, row_kernel, col_kernel):
    n_class = lax.axis_size("parts")
    group = lax.axis_size("sub") * lax.axis_size("pair")
    pages = prepare(counts, probs.T, defocus[None], classes.T, poses.T, spectra)
    other_pages = shift(pages, "pair", 1)
    place = jnp.stack([lax.axis_index("pair"), lax.axis_index("parts")])
    col_rows = jnp.swapaxes(col_kernel, 1, 2)
    parts = insert_particles(place, offsets, row_kernel, col_rows, pages, other_pages, n_class)
    planes = lax.all_gather(sum_at_owner(parts, "parts"), ("sub", "pair"), axis=0, tiled=False)
    mix_rows, mix_cols, last_rows, last_cols = tables(group)
    mine = lax.dynamic_index_in_dim(jnp.asarray(last_cols), lax.axis_index(("sub", "pair")), 1, keepdims=False)
    copies = refine_class(
        planes, jnp.asarray(mix_rows), jnp.asarray(mix_cols), jnp.asarray(last_rows), mine, n_class // NEAR
    )
    return from_all(copies, "parts").astype(F32)


def solution(mesh):
    shards = ("groups", "parts", "pair")
    placed = (
        P(shards, None, None),
        P(shards),
        P(shards, None),
        P(shards, None),
        P(shards, None),
        P(shards),
        P(),
        P(None, "sub", None),
        P(),
    )
    return jax.shard_map(
        per_device,
        mesh=mesh,
        in_specs=placed,
        out_specs=P("groups", ("sub", "pair"), None),
        check_vma=False,
    )
```
